512 devices in a mesh: dap: 128 (over z, y_lo, x, core), seq: 4 (over y_hi).
Axes of the slice: x: 4, y: 8 (y_hi: 4, y_lo: 2; y = y_hi * 2 + y_lo), z: 8, core: 2. Of those that a mesh axis runs over, the one named last changes fastest.
Arguments:
- homolog_tensor: bfloat16 [128, 512, 256], P('dap', 'seq'), may hold values from -6 to 6
- pair_features: bfloat16 [512, 512, 128], P('seq', 'dap'), may hold values from -6 to 6
- entry_real_mask: int32 [128, 512], P('dap', 'seq'), may hold values 0 or 1
- chain_ids: int32 [512], replicated, may hold values from 0 to 3, never falling along the last dimension, each value on 1 to 256 neighbouring positions
- horizontal_matrices: bfloat16 [256, 1024], replicated, may hold values from -0.375 to 0.375
- horizontal_projector: bfloat16 [256, 256], replicated, may hold values from -0.375 to 0.375
- bias_proj: float32 [128, 8], replicated, may hold values from -35.35534 to 35.35534
- chain_bias: float32 [2, 8], replicated, may hold values from -4 to 4
- column_proj: bfloat16 [256, 1024], replicated, may hold values from -12.5 to 12.5
- vertical_projector: bfloat16 [256, 256], replicated, may hold values from -0.375 to 0.375
- expansion_matrix: bfloat16 [256, 1024], replicated, may hold values from -0.375 to 0.375
- contraction_matrix: bfloat16 [1024, 256], replicated, may hold values from -0.1875 to 0.1875
Outputs:
- updated: bfloat16 [128, 512, 256], P('dap', 'seq')
The draws below stay inside these ranges and needn't reach their ends.
Inputs may be any that keep to these rules, and one draw needn't show every extreme that they name: `chain_ids`: chain numbers never fall along the residues.
All inputs are finite; a program needn't handle non-finite values. No bound on the sum of `entry_real_mask` on one device may be relied on, other than what follows from the above.
Results may differ from the reference program's by a relative error of at most 0.013.
The reference program's roundings to bfloat16 on the way count: a program that leaves them out, or rounds other values in their place, can miss the bound.
Values may be sent and summed in bfloat16 or wider, within the bound.
A program may use at most 64 MiB of HBM per device.

```python
import math
import jax
import jax.numpy as jnp
import numpy as np
from jax import lax

FEATURE_DEPTH = 256
CZ = 128
HEAD_TOTAL = 8
HEAD_DEPTH = 32
EXPANDED_UNITS = 1024
HOMOLOG_COUNT = 128
ASSEMBLY_SITES = 512


def draw_bias_proj(key, part):
    starting_tensor = jnp.clip(jax.random.normal(jax.random.fold_in(key, 11), (CZ, HEAD_TOTAL), jnp.float32), -5.0, 5.0) * CZ ** (-0.5)
    return starting_tensor


def draw_column_proj(key, part):
    expanded_dimension = HEAD_TOTAL * HEAD_DEPTH
    starting_tensor = jnp.clip(jax.random.normal(jax.random.fold_in(key, 21), (FEATURE_DEPTH, 4 * expanded_dimension), jnp.float32), -5.0, 5.0) * FEATURE_DEPTH ** (-0.5)
    return starting_tensor.astype(jnp.bfloat16)


def touch_ends(array, rng, smallest, top_value):
    index_at = [jax.random.randint(jax.random.fold_in(rng, axis), (), 0, length) for axis, length in enumerate(array.shape)]
    main_axis = array.shape.index(max(array.shape))
    next_to = index_at[:main_axis] + [(index_at[main_axis] + 1) % array.shape[main_axis]] + index_at[main_axis + 1:]
    return array.at[tuple(index_at)].set(smallest).at[tuple(next_to)].set(top_value)


def block_levels(key, dims, split, least, high):
    loudness, own = 1.0, jax.random.fold_in(key, 6)
    for position, parts in split:
        steps = jnp.exp(jax.random.uniform(jax.random.fold_in(own, position), (parts,), jnp.float32, least / len(split), high / len(split)))
        loudness = loudness * jnp.repeat(steps, dims[position] // parts).reshape([-1 if axis == position else 1 for axis in range(len(dims))])
    return loudness


def profile(amount, total, bound, lean):
    weights = [(1 << 20) // math.isqrt(rank ** lean) + 1 for rank in range(2, amount + 1)]
    spare, holding = total - bound - (amount - 1), [1] * (amount - 1)
    while spare > 0:
        free = [i for i in range(amount - 1) if holding[i] < bound]
        whole, left = sum([weights[i] for i in free]), spare
        for i in free:
            addition = min(bound - holding[i], max(1, left * weights[i] // whole), spare)
            holding[i] = holding[i] + addition
            spare = spare - addition
    return np.array([bound] + holding)


def uneven(stream_key, amount, total, limit, slope):
    if amount == 2:
        one = jax.random.randint(stream_key, (), max(1, total - limit), min(limit, total - 1) + 1)
        return jnp.stack([one, total - one])
    lengths = jnp.asarray(profile(amount, total, limit, slope), jnp.int32)
    pairs = (amount - 1) // 2
    giver, taker = lengths[1:1 + 2 * pairs:2], lengths[2:2 + 2 * pairs:2]
    room = jnp.minimum(giver - 1, limit - taker)
    shifted = jax.random.randint(jax.random.fold_in(stream_key, 1), (pairs,), 0, 1 << 20) % (room + 1)
    lengths = lengths.at[1:1 + 2 * pairs:2].set(giver - shifted).at[2:2 + 2 * pairs:2].set(taker + shifted)
    return lengths[jax.random.permutation(jax.random.fold_in(stream_key, 2), amount)]


def centred(stream_key, dims, scale, limit, pieces=(), kind=jnp.bfloat16):
    gain = block_levels(stream_key, dims, pieces, -0.22, 0.18) if pieces else 1.0
    array = jax.random.normal(stream_key, dims, jnp.float32) * scale * gain
    return jnp.minimum(jnp.maximum(array, -limit), limit).astype(kind)


def setup_inputs(seed: int = 0) -> dict:
    splits = jax.random.split(jax.random.key(seed), 13)
    homolog_tensor = centred(splits[0], (HOMOLOG_COUNT, ASSEMBLY_SITES, FEATURE_DEPTH), 1.0, 6.0, ((0, 128), (1, 4)))
    pair_features = centred(splits[1], (ASSEMBLY_SITES, ASSEMBLY_SITES, CZ), 1.0, 6.0, ((0, 4), (1, 128)))
    entry_real_mask = touch_ends((jax.random.randint(splits[2], (HOMOLOG_COUNT, ASSEMBLY_SITES), 0, 8) < 7).astype(jnp.int32), jax.random.fold_in(splits[2], 1), 0, 1)
    chain_ids = jnp.searchsorted(jnp.cumsum(uneven(splits[3], 4, ASSEMBLY_SITES, ASSEMBLY_SITES // 2, 0)), jnp.arange(ASSEMBLY_SITES), side="right").astype(jnp.int32)
    horizontal_matrices = centred(splits[4], (FEATURE_DEPTH, 4 * HEAD_TOTAL * HEAD_DEPTH), FEATURE_DEPTH ** -0.5, 0.375)
    horizontal_projector = centred(splits[5], (HEAD_TOTAL * HEAD_DEPTH, FEATURE_DEPTH), (HEAD_TOTAL * HEAD_DEPTH) ** -0.5, 0.375)
    bias_proj = draw_bias_proj(jax.random.fold_in(splits[12], 71), 0)
    chain_bias = centred(splits[7], (2, HEAD_TOTAL), 1.0, 4.0, (), jnp.float32)
    column_proj = draw_column_proj(jax.random.fold_in(splits[12], 71), 0)
    vertical_projector = centred(splits[9], (HEAD_TOTAL * HEAD_DEPTH, FEATURE_DEPTH), (HEAD_TOTAL * HEAD_DEPTH) ** -0.5, 0.375)
    expansion_matrix = centred(splits[10], (FEATURE_DEPTH, EXPANDED_UNITS), FEATURE_DEPTH ** -0.5, 0.375)
    contraction_matrix = centred(splits[11], (EXPANDED_UNITS, FEATURE_DEPTH), EXPANDED_UNITS ** -0.5, 0.1875)
    return dict(homolog_tensor=homolog_tensor, pair_features=pair_features, entry_real_mask=entry_real_mask, chain_ids=chain_ids, horizontal_matrices=horizontal_matrices, horizontal_projector=horizontal_projector, bias_proj=bias_proj, chain_bias=chain_bias, column_proj=column_proj, vertical_projector=vertical_projector, expansion_matrix=expansion_matrix, contraction_matrix=contraction_matrix)


epsilon = 1e-05

def layer_norm(inputs):
    center = inputs - lax.optimization_barrier(jnp.mean(inputs, axis=-1, keepdims=True))
    spread = lax.optimization_barrier(jnp.mean(center * center, axis=-1, keepdims=True))
    return center * lax.rsqrt(spread + epsilon)

def attend(queries, key_part, value_part, keep_mask, bias_term):
    scores = jnp.einsum('ihd,jhd->hij', queries.astype(jnp.float32), key_part.astype(jnp.float32)) * HEAD_DEPTH ** (-0.5)
    if bias_term is not None:
        scores = scores + bias_term.astype(jnp.float32)
    scores = jnp.where(keep_mask[None, None, :] > 0, scores, -1000000000.0)
    weights = jax.nn.softmax(scores, axis=-1).astype(jnp.bfloat16)
    return jnp.einsum('hij,jhd->ihd', weights.astype(jnp.float32), value_part.astype(jnp.float32))

def column_update(column, keep_column, column_proj, vertical_projector, expansion_matrix, contraction_matrix):
    expanded_dimension = HEAD_TOTAL * HEAD_DEPTH
    standardized = layer_norm(column.astype(jnp.float32)).astype(jnp.bfloat16)
    projected = jnp.dot(standardized, column_proj, preferred_element_type=jnp.float32).astype(jnp.bfloat16)
    queries = projected[:, :expanded_dimension].reshape(-1, HEAD_TOTAL, HEAD_DEPTH)
    key_part = projected[:, expanded_dimension:2 * expanded_dimension].reshape(-1, HEAD_TOTAL, HEAD_DEPTH)
    value_part = projected[:, 2 * expanded_dimension:3 * expanded_dimension].reshape(-1, HEAD_TOTAL, HEAD_DEPTH)
    attended = attend(queries, key_part, value_part, keep_column, None).reshape(-1, expanded_dimension)
    sigmoid_scaled = (jax.nn.sigmoid(projected[:, 3 * expanded_dimension:].astype(jnp.float32)) * attended).astype(jnp.bfloat16)
    mixed = column.astype(jnp.float32) + jnp.dot(sigmoid_scaled, vertical_projector, preferred_element_type=jnp.float32)
    inner = jnp.maximum(jnp.dot(layer_norm(mixed).astype(jnp.bfloat16), expansion_matrix, preferred_element_type=jnp.float32), 0.0).astype(jnp.bfloat16)
    return (mixed + jnp.dot(inner, contraction_matrix, preferred_element_type=jnp.float32)).astype(jnp.bfloat16)

def reference(homolog_tensor, pair_features, entry_real_mask, chain_ids, horizontal_matrices, horizontal_projector, bias_proj, chain_bias, column_proj, vertical_projector, expansion_matrix, contraction_matrix):
    expanded_dimension = HEAD_TOTAL * HEAD_DEPTH
    normed_pair = layer_norm(pair_features.astype(jnp.float32))
    projected_pair = jnp.einsum('ijc,ch->hij', normed_pair, bias_proj, precision=lax.Precision.HIGHEST)
    same_chain = (chain_ids[:, None] == chain_ids[None, :]).astype(jnp.float32)
    chain_term = chain_bias[0][:, None, None] * same_chain + chain_bias[1][:, None, None] * (1.0 - same_chain)
    pair_bias = (projected_pair + chain_term).astype(jnp.bfloat16)
    standardized = layer_norm(homolog_tensor.astype(jnp.float32)).astype(jnp.bfloat16)
    horizontal_quadruple = jnp.dot(standardized.reshape(-1, FEATURE_DEPTH), horizontal_matrices, preferred_element_type=jnp.float32).astype(jnp.bfloat16).reshape(HOMOLOG_COUNT, ASSEMBLY_SITES, 4 * expanded_dimension)

    def one_row(inputs_row):
        row_values, row_keep = inputs_row
        queries = row_values[:, :expanded_dimension].reshape(ASSEMBLY_SITES, HEAD_TOTAL, HEAD_DEPTH)
        key_part = row_values[:, expanded_dimension:2 * expanded_dimension].reshape(ASSEMBLY_SITES, HEAD_TOTAL, HEAD_DEPTH)
        value_part = row_values[:, 2 * expanded_dimension:3 * expanded_dimension].reshape(ASSEMBLY_SITES, HEAD_TOTAL, HEAD_DEPTH)
        return attend(queries, key_part, value_part, row_keep, pair_bias).reshape(ASSEMBLY_SITES, expanded_dimension)
    attended = lax.map(one_row, (horizontal_quadruple, entry_real_mask))
    sigmoid_scaled = (jax.nn.sigmoid(horizontal_quadruple[..., 3 * expanded_dimension:].astype(jnp.float32)) * attended).astype(jnp.bfloat16)
    leading_homolog = (homolog_tensor.astype(jnp.float32) + jnp.dot(sigmoid_scaled.reshape(-1, expanded_dimension), horizontal_projector, preferred_element_type=jnp.float32).reshape(HOMOLOG_COUNT, ASSEMBLY_SITES, FEATURE_DEPTH)).astype(jnp.bfloat16)

    def single_column(inputs_col):
        return column_update(inputs_col[0], inputs_col[1], column_proj, vertical_projector, expansion_matrix, contraction_matrix)
    output_list = lax.map(single_column, (jnp.swapaxes(leading_homolog, 0, 1), jnp.swapaxes(entry_real_mask, 0, 1)))
    return jnp.swapaxes(output_list, 0, 1)
```

```python
import jax
import jax.numpy as jnp
from jax import lax
from jax.experimental import pallas as pl
from jax.experimental.pallas import tpu as pltpu
from jax.sharding import Mesh
from jax.sharding import PartitionSpec as P

HEADS = 8
DEPTH = 32
WIDE = 256
SCALE = DEPTH ** (-0.5)
EPS = 1e-05
DAP = ("dap_0", "dap_1", "dap_2", "dap_3")
MESH = pl.DeviceIdType.MESH
F32 = jnp.float32
BF16 = jnp.bfloat16


def layer_norm(x):
    center = x - jnp.mean(x, axis=-1, keepdims=True)
    spread = jnp.mean(center * center, axis=-1, keepdims=True)
    return center * lax.rsqrt(spread + EPS)


def mm(a, b):
    return jnp.dot(a, b, preferred_element_type=F32)


def plane_id(k):
    return {"dap_1": lax.div(k, 8), "dap_2": lax.rem(lax.div(k, 2), 4), "dap_3": lax.rem(k, 2)}


def kernel(
    hom, pair, mask, chain_v, bproj, chain_s, cbias, wh_h, ph_h, wc_h, pv_h, ex_h, co_h,
    out,
    wh, ph, wc, pv, ex, co,
    xs, plane, biasall, homall, mrow, mcol, keep, keepc,
    qbd, vt, scores, ot, gt,
    a1, a2s, a2, b1s, b1, b2s, b2, fs,
    wsem, plane_s, plane_r, hom_s, hom_r, mrow_s, mrow_r, mp_s, mp_r, mz_s, mz_r,
    ring_s, ring_r, part_s, part_r, a1_s, a1_r, a2_ss, a2_r, b1_ss, b1_r, b2_ss, b2_r,
):
    z = lax.axis_index("dap_0")
    y = lax.axis_index("dap_1")
    x = lax.axis_index("dap_2")
    c = lax.axis_index("dap_3")
    seq = lax.axis_index("seq")
    k = y * 8 + x * 2 + c
    dap = z * 16 + k

    loads = [pltpu.make_async_copy(s, d, wsem.at[n]) for n, (s, d) in enumerate(
        ((wh_h, wh), (ph_h, ph), (wc_h, wc), (pv_h, pv), (ex_h, ex), (co_h, co)))]
    for ld in loads:
        ld.start()

    def remote(src, dst, ss, rs, device):
        return pltpu.make_async_remote_copy(
            src_ref=src, dst_ref=dst, send_sem=ss, recv_sem=rs, device_id=device,
            device_id_type=MESH)

    barrier = pltpu.get_barrier_semaphore()

    @pl.loop(1, 16)
    def _(p):
        pl.semaphore_signal(barrier, inc=1, device_id=plane_id(lax.rem(k + p, 16)), device_id_type=MESH)

    @pl.loop(1, 8)
    def _(p):
        pl.semaphore_signal(barrier, inc=1, device_id={"dap_0": lax.rem(z + p, 8)}, device_id_type=MESH)

    @pl.loop(1, 4)
    def _(p):
        pl.semaphore_signal(barrier, inc=1, device_id={"seq": lax.rem(seq + p, 4)}, device_id_type=MESH)

    xs[...] = layer_norm(pair[...].astype(F32))
    bt = bproj[...].T
    head = lax.broadcasted_iota(jnp.int32, (8, 128), 0)
    cb0 = jnp.zeros((8, 128), F32)
    cb1 = jnp.zeros((8, 128), F32)
    for h in range(HEADS):
        cb0 = jnp.where(head == h, cbias[h], cb0)
        cb1 = jnp.where(head == h, cbias[HEADS + h], cb1)
    row_chain = jnp.broadcast_to(chain_v[pl.ds(seq, 1), :], (8, 128))
    parts = []
    for j in range(4):
        xj = xs[pl.ds(j, 128, stride=4), :]
        pj = lax.dot_general(bt, xj, (((1,), (1,)), ((), ())), precision=lax.Precision.HIGHEST,
                             preferred_element_type=F32)
        parts.append(pj + jnp.where(row_chain == chain_s[dap * 4 + j], cb0, cb1))
    plane[k] = jnp.concatenate(parts, axis=0).astype(BF16)
    homall[seq] = hom[...]
    mrow[seq] = mask[...]
    mcol[z, k] = mask[...]
    qbd[...] = jnp.zeros_like(qbd)

    pl.semaphore_wait(barrier, 25)

    def plane_copy(p):
        to = lax.rem(k + p, 16)
        return remote(plane.at[k], plane.at[k], plane_s.at[to], plane_r.at[k], plane_id(to))

    def plane_recv(p):
        fr = lax.rem(k + p, 16)
        return remote(plane.at[fr], plane.at[fr], plane_s.at[fr], plane_r.at[fr], plane_id(fr))

    def hom_copy(p):
        to = lax.rem(seq + p, 4)
        return remote(hom, homall.at[seq], hom_s.at[to], hom_r.at[seq], {"seq": to})

    def hom_recv(p):
        fr = lax.rem(seq + p, 4)
        return remote(hom, homall.at[fr], hom_s.at[fr], hom_r.at[fr], {"seq": fr})

    def mrow_copy(p):
        to = lax.rem(seq + p, 4)
        return remote(mask, mrow.at[seq], mrow_s.at[to], mrow_r.at[seq], {"seq": to})

    def mrow_recv(p):
        fr = lax.rem(seq + p, 4)
        return remote(mask, mrow.at[fr], mrow_s.at[fr], mrow_r.at[fr], {"seq": fr})

    def mp_copy(p):
        to = lax.rem(k + p, 16)
        return remote(mask, mcol.at[z, k], mp_s.at[to], mp_r.at[k], plane_id(to))

    def mp_recv(p):
        fr = lax.rem(k + p, 16)
        return remote(mask, mcol.at[z, fr], mp_s.at[fr], mp_r.at[fr], plane_id(fr))

    def mz_copy(p):
        to = lax.rem(z + p, 8)
        return remote(mcol.at[z], mcol.at[z], mz_s.at[to], mz_r.at[z], {"dap_0": to})

    def mz_recv(p):
        fr = lax.rem(z + p, 8)
        return remote(mcol.at[fr], mcol.at[fr], mz_s.at[fr], mz_r.at[fr], {"dap_0": fr})

    pl.loop(1, 16)(lambda p: plane_copy(p).start())
    pl.loop(1, 4)(lambda p: mrow_copy(p).start())
    pl.loop(1, 4)(lambda p: hom_copy(p).start())
    pl.loop(1, 16)(lambda p: mp_copy(p).start())

    def transposed(v):
        return v.astype(BF16).T

    def spread_queries(qt):
        for h in range(HEADS):
            qbd[h * 32:(h + 1) * 32, h * 128:(h + 1) * 128] = qt[h * 32:(h + 1) * 32, :]

    def block_scores(b, keys, values):
        scores[pl.ds(pl.multiple_of(b * 128, 128), 128), :] = mm(keys.astype(BF16), qbd[...])
        vt[:, pl.ds(pl.multiple_of(b * 128, 128), 128)] = transposed(values)

    loads[0].wait()
    own = hom[...].astype(F32)
    qkvg = mm(layer_norm(own).astype(BF16), wh[...])
    spread_queries(transposed(qkvg[:, :WIDE]))
    gt[...] = transposed(qkvg[:, 3 * WIDE:]).astype(F32)
    block_scores(seq, qkvg[:, WIDE:2 * WIDE], qkvg[:, 2 * WIDE:3 * WIDE])

    def neighbour_block(p):
        b = lax.rem(seq + p, 4)
        hom_recv(p).wait_recv()
        kv = mm(layer_norm(homall[b].astype(F32)).astype(BF16), wh[:, WIDE:3 * WIDE])
        block_scores(b, kv[:, :WIDE], kv[:, WIDE:])

    pl.loop(1, 16)(lambda p: plane_recv(p).wait_recv())
    xs[...] = plane[...].reshape(512, 128).astype(F32)
    for h in range(HEADS):
        biasall[z, :, h * 128:(h + 1) * 128] = xs[pl.ds(h, 64, stride=8), :].astype(BF16)

    step = 1 - 2 * c
    onward = {"dap_0": lax.rem(z + step + 8, 8)}
    partner = {"dap_3": 1 - c}

    def piece(block, q):
        return biasall.at[block, pl.ds(pl.multiple_of(q * 32, 32), 32)]

    def ring_copy(s, i):
        b = lax.rem(z - step * s + 8, 8)
        ref = piece(b, lax.rem(c + i, 2))
        return remote(ref, ref, ring_s.at[s, i], ring_r.at[s, i], onward)

    def ring_recv(s, i):
        b = lax.rem(z - step * (s + 1) + 8, 8)
        ref = piece(b, lax.rem(c + i, 2))
        return remote(ref, ref, ring_s.at[s, i], ring_r.at[s, i], onward)

    def part_copy(s, i):
        b = lax.rem(z - step * (s + 1) + 8, 8)
        ref = piece(b, lax.rem(c + i, 2))
        return remote(ref, ref, part_s.at[s, i], part_r.at[s, i], partner)

    def part_recv(s, i):
        b = lax.rem(z + step * (s + 1) + 8, 8)
        ref = piece(b, lax.rem(1 - c + i, 2))
        return remote(ref, ref, part_s.at[s, i], part_r.at[s, i], partner)

    hops = [(s, i) for s in range(4) for i in range(2) if s < 3 or i == 0]
    for i in range(2):
        ring_copy(0, i).start()
    pl.loop(1, 16)(lambda p: mp_recv(p).wait_recv())
    pl.loop(1, 8)(lambda p: mz_copy(p).start())
    for s, i in hops:
        ring_recv(s, i).wait_recv()
        if (s + 1, i) in hops:
            ring_copy(s + 1, i).start()
        part_copy(s, i).start()
        if (s, i) == (0, 1):
            neighbour_block(1)
            neighbour_block(3)
        if (s, i) == (1, 1):
            neighbour_block(2)
            pl.loop(1, 4)(lambda p: mrow_recv(p).wait_recv())
            for b in range(4):
                keep[b * 128:(b + 1) * 128, :] = jnp.broadcast_to(mrow[b].astype(F32), (128, 128)).T
        if (s, i) == (2, 0):
            pl.loop(1, 8)(lambda p: mz_recv(p).wait_recv())
            fs[:128, :] = mcol[...].reshape(128, 128).astype(F32)
            pick = (lax.broadcasted_iota(jnp.int32, (128, 128), 0) == dap).astype(BF16)
            rows = [fs[pl.ds(n, 8, stride=16), :] for n in range(16)]
            keepc[...] = mm(jnp.concatenate(rows, axis=0).astype(BF16), pick)
    for s, i in hops:
        part_recv(s, i).wait_recv()

    def softmax_out(s, vth):
        m = jnp.max(s, axis=0, keepdims=True)
        e = jnp.exp(s - m)
        w = (e * (1.0 / jnp.sum(e, axis=0, keepdims=True))).astype(BF16)
        return mm(vth, w)

    for h in range(HEADS):
        lanes = slice(h * 128, (h + 1) * 128)
        s = scores[:, lanes] * SCALE + biasall[:, :, lanes].reshape(512, 128).astype(F32)
        s = jnp.where(keep[...] > 0.0, s, -1000000000.0)
        ot[h * 32:(h + 1) * 32, :] = softmax_out(s, vt[h * 32:(h + 1) * 32, :])

    def split(v):
        fs[:128, :] = v[:, :128].astype(F32)
        fs[128:, :] = v[:, 128:].astype(F32)

    def gated_project(w):
        g = (jax.nn.sigmoid(gt[...]) * ot[...]).astype(BF16)
        return mm(g.T, w)

    loads[1].wait()
    one = (hom[...].astype(F32) + gated_project(ph[...])).astype(BF16)
    b2s[...] = one.reshape(8, 16, WIDE)
    a1[z] = b2s[z]

    def a1_copy(p):
        to = lax.rem(z + p, 8)
        return remote(b2s.at[to], a1.at[z], a1_s.at[to], a1_r.at[z], {"dap_0": to})

    def a1_recv(p):
        fr = lax.rem(z + p, 8)
        return remote(b2s.at[fr], a1.at[fr], a1_s.at[fr], a1_r.at[fr], {"dap_0": fr})

    pl.loop(1, 8)(lambda p: a1_copy(p).start())
    pl.loop(1, 8)(lambda p: a1_recv(p).wait_recv())

    split(a1[...].reshape(128, WIDE))
    for n in range(16):
        for t in range(2):
            a2s[n, :, t * 128:(t + 1) * 128] = fs[pl.ds(t * 128 + n, 8, stride=16), :].astype(BF16)
    a2[k] = a2s[k]

    def a2_copy(p):
        to = lax.rem(k + p, 16)
        return remote(a2s.at[to], a2.at[k], a2_ss.at[to], a2_r.at[k], plane_id(to))

    def a2_recv(p):
        fr = lax.rem(k + p, 16)
        return remote(a2s.at[fr], a2.at[fr], a2_ss.at[fr], a2_r.at[fr], plane_id(fr))

    pl.loop(1, 16)(lambda p: a2_copy(p).start())
    loads[2].wait()
    loads[3].wait()
    loads[4].wait()
    loads[5].wait()
    pl.loop(1, 16)(lambda p: a2_recv(p).wait_recv())

    col = a2[...].astype(F32).reshape(128, WIDE)
    qkvg = mm(layer_norm(col).astype(BF16), wc[...])
    spread_queries(transposed(qkvg[:, :WIDE]))
    gt[...] = transposed(qkvg[:, 3 * WIDE:]).astype(F32)
    cs = mm(qkvg[:, WIDE:2 * WIDE].astype(BF16), qbd[...]) * SCALE
    cvt = transposed(qkvg[:, 2 * WIDE:3 * WIDE])
    for h in range(HEADS):
        s = jnp.where(keepc[...] > 0.0, cs[:, h * 128:(h + 1) * 128], -1000000000.0)
        ot[h * 32:(h + 1) * 32, :] = softmax_out(s, cvt[h * 32:(h + 1) * 32, :])
    two = col + gated_project(pv[...])
    inner = jnp.maximum(mm(layer_norm(two).astype(BF16), ex[...]), 0.0).astype(BF16)
    done = two + mm(inner, co[...])
    b1s[...] = done.reshape(16, 8, WIDE).astype(BF16)
    b1[k] = b1s[k]

    def b1_copy(p):
        to = lax.rem(k + p, 16)
        return remote(b1s.at[to], b1.at[k], b1_ss.at[to], b1_r.at[k], plane_id(to))

    def b1_recv(p):
        fr = lax.rem(k + p, 16)
        return remote(b1s.at[fr], b1.at[fr], b1_ss.at[fr], b1_r.at[fr], plane_id(fr))

    pl.loop(1, 16)(lambda p: b1_copy(p).start())
    pl.loop(1, 8)(lambda p: a1_copy(p).wait_send())
    pl.loop(1, 16)(lambda p: b1_recv(p).wait_recv())
    split(b1[...].astype(F32).reshape(128, WIDE))
    for n in range(8):
        for t in range(2):
            b2s[n, :, t * 128:(t + 1) * 128] = fs[pl.ds(t * 128 + n, 16, stride=8), :].astype(BF16)
    b2[z] = b2s[z]

    def b2_copy(p):
        to = lax.rem(z + p, 8)
        return remote(b2s.at[to], b2.at[z], b2_ss.at[to], b2_r.at[z], {"dap_0": to})

    def b2_recv(p):
        fr = lax.rem(z + p, 8)
        return remote(b2s.at[fr], b2.at[fr], b2_ss.at[fr], b2_r.at[fr], {"dap_0": fr})

    pl.loop(1, 8)(lambda p: b2_copy(p).start())

    pl.loop(1, 16)(lambda p: plane_copy(p).wait_send())
    pl.loop(1, 16)(lambda p: mp_copy(p).wait_send())
    pl.loop(1, 16)(lambda p: a2_copy(p).wait_send())
    pl.loop(1, 16)(lambda p: b1_copy(p).wait_send())
    pl.loop(1, 8)(lambda p: mz_copy(p).wait_send())
    pl.loop(1, 4)(lambda p: hom_copy(p).wait_send())
    pl.loop(1, 4)(lambda p: mrow_copy(p).wait_send())
    for s, i in hops:
        ring_copy(s, i).wait_send()
        part_copy(s, i).wait_send()

    pl.loop(1, 8)(lambda p: b2_recv(p).wait_recv())
    pl.loop(1, 8)(lambda p: b2_copy(p).wait_send())
    out[...] = b2[...].reshape(128, WIDE)


def body(
    homolog_tensor, pair_features, entry_real_mask, chain_ids, horizontal_matrices,
    horizontal_projector, bias_proj, chain_bias, column_proj, vertical_projector,
    expansion_matrix, contraction_matrix,
):
    vmem = pl.BlockSpec(memory_space=pltpu.VMEM)
    smem = pl.BlockSpec(memory_space=pltpu.SMEM)
    hbm = pl.BlockSpec(memory_space=pl.ANY)
    dma = pltpu.SemaphoreType.DMA
    updated = pl.pallas_call(
        kernel,
        name="msa_block",
        out_shape=jax.ShapeDtypeStruct((128, WIDE), BF16),
        in_specs=[vmem] * 5 + [smem] * 2 + [hbm] * 6,
        out_specs=vmem,
        scratch_shapes=[
            pltpu.VMEM((WIDE, 4 * WIDE), BF16),
            pltpu.VMEM((WIDE, WIDE), BF16),
            pltpu.VMEM((WIDE, 4 * WIDE), BF16),
            pltpu.VMEM((WIDE, WIDE), BF16),
            pltpu.VMEM((WIDE, 4 * WIDE), BF16),
            pltpu.VMEM((4 * WIDE, WIDE), BF16),
            pltpu.VMEM((512, 128), F32),
            pltpu.VMEM((16, 32, 128), BF16),
            pltpu.VMEM((8, 64, 1024), BF16),
            pltpu.VMEM((4, 128, WIDE), BF16),
            pltpu.VMEM((4, 1, 128), jnp.int32),
            pltpu.VMEM((8, 16, 1, 128), jnp.int32),
            pltpu.VMEM((512, 128), F32),
            pltpu.VMEM((128, 128), F32),
            pltpu.VMEM((WIDE, 1024), BF16),
            pltpu.VMEM((WIDE, 512), BF16),
            pltpu.VMEM((512, 1024), F32),
            pltpu.VMEM((WIDE, 128), F32),
            pltpu.VMEM((WIDE, 128), F32),
            pltpu.VMEM((8, 16, WIDE), BF16),
            pltpu.VMEM((16, 8, WIDE), BF16),
            pltpu.VMEM((16, 8, WIDE), BF16),
            pltpu.VMEM((16, 8, WIDE), BF16),
            pltpu.VMEM((16, 8, WIDE), BF16),
            pltpu.VMEM((8, 16, WIDE), BF16),
            pltpu.VMEM((8, 16, WIDE), BF16),
            pltpu.VMEM((256, 128), F32),
            dma((6,)), dma((16,)), dma((16,)), dma((4,)), dma((4,)), dma((4,)), dma((4,)),
            dma((16,)), dma((16,)), dma((8,)), dma((8,)),
            dma((4, 2)), dma((4, 2)), dma((4, 2)), dma((4, 2)),
            dma((8,)), dma((8,)), dma((16,)), dma((16,)), dma((16,)), dma((16,)), dma((8,)), dma((8,)),
        ],
        compiler_params=pltpu.CompilerParams(collective_id=0, has_side_effects=True),
    )(
        homolog_tensor.reshape(128, WIDE),
        pair_features.reshape(512, 128),
        entry_real_mask,
        chain_ids.reshape(4, 128),
        bias_proj,
        chain_ids,
        chain_bias.reshape(16),
        horizontal_matrices,
        horizontal_projector,
        column_proj,
        vertical_projector,
        expansion_matrix,
        contraction_matrix,
    )
    return updated.reshape(1, 128, WIDE)


def solution(mesh):
    torus = Mesh(
        mesh.devices.reshape(8, 2, 4, 2, mesh.shape["seq"]),
        ("dap_0", "dap_1", "dap_2", "dap_3", "seq"),
    )
    return jax.shard_map(
        body,
        mesh=torus,
        in_specs=(P(DAP, "seq", None), P("seq", DAP, None), P(DAP, "seq")) + (P(),) * 9,
        out_specs=P(DAP, "seq", None),
        check_vma=False,
    )
```

```python
import jax
import jax.numpy as jnp
from jax import lax
from jax.experimental import pallas as pl
from jax.experimental.pallas import tpu as pltpu
from jax.sharding import Mesh
from jax.sharding import PartitionSpec as P

HEADS = 8
DEPTH = 32
WIDE = 256
SCALE = DEPTH ** (-0.5)
EPS = 1e-05
DAP = ("dap_0", "dap_1", "dap_2", "dap_3")
MESH = pl.DeviceIdType.MESH
F32 = jnp.float32
BF16 = jnp.bfloat16


def layer_norm(x):
    center = x - jnp.mean(x, axis=-1, keepdims=True)
    spread = jnp.mean(center * center, axis=-1, keepdims=True)
    return center * lax.rsqrt(spread + EPS)


def mm(a, b):
    return jnp.dot(a, b, preferred_element_type=F32)


def plane_id(k):
    return {"dap_1": lax.div(k, 8), "dap_2": lax.rem(lax.div(k, 2), 4), "dap_3": lax.rem(k, 2)}


def kernel(
    hom_h, pair_h, mask_h, chain_h, bproj_h, cbias_h, wh_h, ph_h, wc_h, pv_h, ex_h, co_h,
    out,
    pair, chain, bproj, cbias, wh, ph, wc, pv, ex, co,
    xs, mine, plane, biasall, homall, mrow, mcol, keep, keepc,
    qbd, vt, scores, ot, gt,
    a1, a2s, a2, b1s, b1, b2s, b2, fs,
    lsem, plane_s, plane_r, hom_s, hom_r, mrow_s, mrow_r, mp_s, mp_r, mz_s, mz_r,
    ring_s, ring_r, part_s, part_r, a1_s, a1_r, a2_s, a2_r, b1_s, b1_r, b2_s, b2_r,
):
    z = lax.axis_index("dap_0")
    y = lax.axis_index("dap_1")
    x = lax.axis_index("dap_2")
    c = lax.axis_index("dap_3")
    seq = lax.axis_index("seq")
    k = y * 8 + x * 2 + c
    dap = z * 16 + k

    def local(n, src, dst):
        return pltpu.make_async_copy(src, dst, lsem.at[n])

    l_pair = local(0, pair_h, pair)
    l_chain = local(1, chain_h, chain)
    l_bproj = local(2, bproj_h, bproj)
    l_cbias = local(3, cbias_h, cbias)
    l_hom = local(4, hom_h, homall.at[seq])
    l_mrow = local(5, mask_h, mrow.at[seq])
    l_mcol = local(6, mask_h, mcol.at[z, k])
    l_wh = local(7, wh_h, wh)
    l_rest = [local(8 + n, a, b) for n, (a, b) in enumerate(
        ((ph_h, ph), (wc_h, wc), (pv_h, pv), (ex_h, ex), (co_h, co)))]
    for ld in (l_pair, l_chain, l_bproj, l_cbias, l_hom, l_mrow, l_mcol):
        ld.start()

    def remote(src, dst, ss, rs, device):
        return pltpu.make_async_remote_copy(
            src_ref=src, dst_ref=dst, send_sem=ss, recv_sem=rs, device_id=device,
            device_id_type=MESH)

    barrier = pltpu.get_barrier_semaphore()

    @pl.loop(1, 8)
    def _(p):
        pl.semaphore_signal(barrier, inc=1, device_id={"dap_0": lax.rem(z + p, 8)}, device_id_type=MESH)

    @pl.loop(1, 4)
    def _(p):
        pl.semaphore_signal(barrier, inc=1, device_id={"seq": lax.rem(seq + p, 4)}, device_id_type=MESH)

    @pl.loop(1, 16)
    def _(p):
        pl.semaphore_signal(barrier, inc=1, device_id=plane_id(lax.rem(k + p, 16)), device_id_type=MESH)

    l_wh.start()
    for ld in l_rest:
        ld.start()

    l_chain.wait()
    l_cbias.wait()
    diagonal = (lax.broadcasted_iota(jnp.int32, (8, 8), 0)
                == lax.broadcasted_iota(jnp.int32, (8, 8), 1))

    def by_head(row):
        return jnp.sum(jnp.where(diagonal, jnp.broadcast_to(row, (8, 8)), 0.0), axis=1, keepdims=True)

    cb0 = jnp.broadcast_to(by_head(cbias[0:1, :]), (8, 128))
    cb1 = jnp.broadcast_to(by_head(cbias[1:2, :]), (8, 128))
    row_chain = jnp.broadcast_to(chain[pl.ds(seq, 1), :], (8, 128))
    my_chain = jnp.broadcast_to(chain[pl.ds(lax.div(dap, 32), 1), :], (8, 128))
    lane = lax.broadcasted_iota(jnp.int32, (8, 128), 1) - lax.rem(dap, 32) * 4
    terms = []
    for j in range(4):
        own_chain = jnp.sum(jnp.where(lane == j, my_chain, 0).astype(F32), axis=1, keepdims=True)
        terms.append(jnp.where(row_chain.astype(F32) == own_chain, cb0, cb1))
    with jax.named_scope("waitpair"):
        l_pair.wait()
    xs[...] = layer_norm(pair[...].astype(F32))
    l_bproj.wait()
    parts = []
    for j in range(4):
        xj = xs[pl.ds(j, 128, stride=4), :]
        pj = lax.dot_general(bproj[...], xj, (((1,), (1,)), ((), ())), precision=lax.Precision.HIGHEST,
                             preferred_element_type=F32)
        parts.append(pj + terms[j])
    for g in range(2):
        mine[g] = jnp.concatenate([p[g * 4:g * 4 + 4] for p in parts], axis=0).astype(BF16)
    plane[k] = mine[c]
    l_hom.wait()
    l_mrow.wait()
    l_mcol.wait()
    qbd[...] = jnp.zeros_like(qbd)

    with jax.named_scope("barrier"):
        pl.semaphore_wait(barrier, 25)

    def plane_copy(p):
        to = lax.rem(k + p, 16)
        return remote(mine.at[lax.rem(to, 2)], plane.at[k], plane_s, plane_r, plane_id(to))

    def hom_copy(p):
        to = lax.rem(seq + p, 4)
        return remote(homall.at[seq], homall.at[seq], hom_s, hom_r.at[seq], {"seq": to})

    def hom_recv(p):
        fr = lax.rem(seq + p, 4)
        return remote(homall.at[fr], homall.at[fr], hom_s, hom_r.at[fr], {"seq": fr})

    def mrow_copy(p):
        to = lax.rem(seq + p, 4)
        return remote(mrow.at[seq], mrow.at[seq], mrow_s, mrow_r, {"seq": to})

    def mp_copy(p):
        to = lax.rem(k + p, 16)
        return remote(mcol.at[z, k], mcol.at[z, k], mp_s, mp_r, plane_id(to))

    def mz_copy(p):
        to = lax.rem(z + p, 8)
        return remote(mcol.at[z], mcol.at[z], mz_s, mz_r, {"dap_0": to})

    def drain(ref, sem):
        pltpu.make_async_copy(ref, ref, sem).wait()

    pl.loop(1, 16)(lambda p: plane_copy(p).start())
    pl.loop(1, 4)(lambda p: mrow_copy(p).start())
    pl.loop(1, 16)(lambda p: mp_copy(p).start())
    pl.loop(1, 4)(lambda p: hom_copy(p).start())

    def transposed(v):
        return v.astype(BF16).T

    def spread_queries(qt):
        for h in range(HEADS):
            qbd[h * 32:(h + 1) * 32, h * 128:(h + 1) * 128] = qt[h * 32:(h + 1) * 32, :]

    def block_scores(b, keys, values):
        scores[pl.ds(pl.multiple_of(b * 128, 128), 128), :] = mm(keys.astype(BF16), qbd[...])
        vt[:, pl.ds(pl.multiple_of(b * 128, 128), 128)] = transposed(values)

    l_wh.wait()
    own = homall[seq].astype(F32)
    with jax.named_scope("ownqkv"):
        qkvg = mm(layer_norm(own).astype(BF16), wh[...])
        spread_queries(transposed(qkvg[:, :WIDE]))
        gt[...] = transposed(qkvg[:, 3 * WIDE:]).astype(F32)
        block_scores(seq, qkvg[:, WIDE:2 * WIDE], qkvg[:, 2 * WIDE:3 * WIDE])

    def neighbour_block(p):
        b = lax.rem(seq + p, 4)
        with jax.named_scope(f"hom{p}"):
            hom_recv(p).wait_recv()
        kv = mm(layer_norm(homall[b].astype(F32)).astype(BF16), wh[:, WIDE:3 * WIDE])
        block_scores(b, kv[:, :WIDE], kv[:, WIDE:])

    with jax.named_scope("waitplane"):
        drain(plane.at[pl.ds(0, 15)], plane_r)
    xs[:256, :] = plane[...].reshape(256, 128).astype(F32)
    for h in range(4):
        biasall[c, z, :, h * 128:(h + 1) * 128] = xs[pl.ds(h, 64, stride=4), :].astype(BF16)

    steps = (1, 7)
    partner = {"dap_3": 1 - c}

    def piece(half, block, i):
        return biasall.at[half, block, pl.ds(i * 32, 32)]

    def ring_copy(d, s, i):
        ref = piece(c, lax.rem(z + (8 - steps[d]) * s, 8), i)
        return remote(ref, ref, ring_s, ring_r.at[d, s, i], {"dap_0": lax.rem(z + steps[d], 8)})

    def ring_recv(d, s, i):
        ref = piece(c, lax.rem(z + (8 - steps[d]) * (s + 1), 8), i)
        return remote(ref, ref, ring_s, ring_r.at[d, s, i], {"dap_0": lax.rem(z + steps[d], 8)})

    def part_copy(d, s, i):
        ref = piece(c, lax.rem(z + (8 - steps[d]) * (s + 1), 8), i)
        return remote(ref, ref, part_s, part_r, partner)

    hops = [(d, s, i) for s in range(4) for i in range(2) for d in range(2) if s < 3 or i == d]
    for i in range(2):
        for d in range(2):
            ring_copy(d, 0, i).start()
    remote(biasall.at[c, z], biasall.at[c, z], part_s, part_r, partner).start()
    with jax.named_scope("nb1"):
        neighbour_block(1)
    for d, s, i in hops:
        with jax.named_scope(f"ring{d}{s}{i}"):
            ring_recv(d, s, i).wait_recv()
        if (d, s + 1, i) in hops:
            ring_copy(d, s + 1, i).start()
        part_copy(d, s, i).start()
        if (d, s, i) == (1, 0, 1):
            with jax.named_scope("waitmp"):
                drain(mcol.at[0, pl.ds(0, 15)], mp_r)
            pl.loop(1, 8)(lambda p: mz_copy(p).start())
            with jax.named_scope("nb3"):
                neighbour_block(3)
        if (d, s, i) == (1, 1, 1):
            with jax.named_scope("nb2"):
                neighbour_block(2)
        if (d, s, i) == (1, 2, 0):
            with jax.named_scope("mask"):
                drain(mrow.at[pl.ds(0, 3)], mrow_r)
                for b in range(4):
                    keep[b * 128:(b + 1) * 128, :] = jnp.broadcast_to(mrow[b].astype(F32), (128, 128)).T
                drain(mcol.at[pl.ds(0, 7)], mz_r)
                fs[:128, :] = mcol[...].reshape(128, 128).astype(F32)
                pick = (lax.broadcasted_iota(jnp.int32, (128, 128), 0) == dap).astype(BF16)
                rows = [fs[pl.ds(n, 8, stride=16), :] for n in range(16)]
                keepc[...] = mm(jnp.concatenate(rows, axis=0).astype(BF16), pick)
    with jax.named_scope("partner"):
        drain(biasall.at[1 - c], part_r)

    def softmax_out(s, vth):
        m = jnp.max(s, axis=0, keepdims=True)
        e = jnp.exp(s - m)
        w = (e * (1.0 / jnp.sum(e, axis=0, keepdims=True))).astype(BF16)
        return mm(vth, w)

    with jax.named_scope("rowattn"):
        for h in range(HEADS):
            lanes = slice(h * 128, (h + 1) * 128)
            s = scores[:, lanes] * SCALE + biasall[h // 4, :, :, (h % 4) * 128:(h % 4 + 1) * 128].reshape(512, 128).astype(F32)
            s = jnp.where(keep[...] > 0.0, s, -1000000000.0)
            ot[h * 32:(h + 1) * 32, :] = softmax_out(s, vt[h * 32:(h + 1) * 32, :])

    def split(v):
        fs[:128, :] = v[:, :128].astype(F32)
        fs[128:, :] = v[:, 128:].astype(F32)

    def gated_project(w):
        g = (jax.nn.sigmoid(gt[...]) * ot[...]).astype(BF16)
        return mm(g.T, w)

    with jax.named_scope("rowproj"):
        l_rest[0].wait()
        one = (homall[seq].astype(F32) + gated_project(ph[...])).astype(BF16)
        b2s[...] = one.reshape(8, 16, WIDE)
        a1[z] = b2s[z]

    def a1_copy(p):
        to = lax.rem(z + p, 8)
        return remote(b2s.at[to], a1.at[z], a1_s, a1_r, {"dap_0": to})

    pl.loop(1, 8)(lambda p: a1_copy(p).start())
    with jax.named_scope("waita1"):
        drain(a1.at[pl.ds(0, 7)], a1_r)

    split(a1[...].reshape(128, WIDE))
    for n in range(16):
        for t in range(2):
            a2s[n, :, t * 128:(t + 1) * 128] = fs[pl.ds(t * 128 + n, 8, stride=16), :].astype(BF16)
    a2[k] = a2s[k]

    def a2_copy(p):
        to = lax.rem(k + p, 16)
        return remote(a2s.at[to], a2.at[k], a2_s, a2_r, plane_id(to))

    pl.loop(1, 16)(lambda p: a2_copy(p).start())
    for ld in l_rest[1:]:
        ld.wait()
    with jax.named_scope("waita2"):
        drain(a2.at[pl.ds(0, 15)], a2_r)

    with jax.named_scope("colattn"):
        col = a2[...].astype(F32).reshape(128, WIDE)
        qkvg = mm(layer_norm(col).astype(BF16), wc[...])
        spread_queries(transposed(qkvg[:, :WIDE]))
        gt[...] = transposed(qkvg[:, 3 * WIDE:]).astype(F32)
        cs = mm(qkvg[:, WIDE:2 * WIDE].astype(BF16), qbd[...]) * SCALE
        cvt = transposed(qkvg[:, 2 * WIDE:3 * WIDE])
        for h in range(HEADS):
            s = jnp.where(keepc[...] > 0.0, cs[:, h * 128:(h + 1) * 128], -1000000000.0)
            ot[h * 32:(h + 1) * 32, :] = softmax_out(s, cvt[h * 32:(h + 1) * 32, :])
    with jax.named_scope("transition"):
        two = col + gated_project(pv[...])
        inner = jnp.maximum(mm(layer_norm(two).astype(BF16), ex[...]), 0.0).astype(BF16)
        done = two + mm(inner, co[...])
        b1s[...] = done.reshape(16, 8, WIDE).astype(BF16)
        b1[k] = b1s[k]

    def b1_copy(p):
        to = lax.rem(k + p, 16)
        return remote(b1s.at[to], b1.at[k], b1_s, b1_r, plane_id(to))

    pl.loop(1, 16)(lambda p: b1_copy(p).start())
    drain(a1.at[pl.ds(0, 7)], a1_s)
    with jax.named_scope("waitb1"):
        drain(b1.at[pl.ds(0, 15)], b1_r)
    split(b1[...].astype(F32).reshape(128, WIDE))
    for n in range(8):
        for t in range(2):
            b2s[n, :, t * 128:(t + 1) * 128] = fs[pl.ds(t * 128 + n, 16, stride=8), :].astype(BF16)
    b2[z] = b2s[z]

    def b2_copy(p):
        to = lax.rem(z + p, 8)
        return remote(b2s.at[to], b2.at[z], b2_s, b2_r, {"dap_0": to})

    pl.loop(1, 8)(lambda p: b2_copy(p).start())

    drain(plane.at[pl.ds(0, 15)], plane_s)
    drain(mcol.at[0, pl.ds(0, 15)], mp_s)
    drain(a2.at[pl.ds(0, 15)], a2_s)
    drain(b1.at[pl.ds(0, 15)], b1_s)
    drain(mcol.at[pl.ds(0, 7)], mz_s)
    drain(homall.at[pl.ds(0, 3)], hom_s)
    drain(mrow.at[pl.ds(0, 3)], mrow_s)
    drain(biasall.at[0, pl.ds(0, 7)], ring_s)
    drain(biasall.at[0], part_s)
    with jax.named_scope("waitb2"):
        drain(b2.at[pl.ds(0, 7)], b2_r)
    with jax.named_scope("tail"):
        drain(b2.at[pl.ds(0, 7)], b2_s)
        out[...] = b2[...].reshape(128, WIDE)


def body(
    homolog_tensor, pair_features, entry_real_mask, chain_ids, horizontal_matrices,
    horizontal_projector, bias_proj, chain_bias, column_proj, vertical_projector,
    expansion_matrix, contraction_matrix,
):
    vmem = pl.BlockSpec(memory_space=pltpu.VMEM)
    hbm = pl.BlockSpec(memory_space=pl.ANY)
    dma = pltpu.SemaphoreType.DMA
    updated = pl.pallas_call(
        kernel,
        name="msa_block",
        out_shape=pltpu.VMEM((128, WIDE), BF16),
        in_specs=[hbm] * 12,
        out_specs=vmem,
        scratch_shapes=[
            pltpu.VMEM((512, 128), BF16),
            pltpu.VMEM((4, 128), jnp.int32),
            pltpu.VMEM((8, 128), F32),
            pltpu.VMEM((2, 8), F32),
            pltpu.VMEM((WIDE, 4 * WIDE), BF16),
            pltpu.VMEM((WIDE, WIDE), BF16),
            pltpu.VMEM((WIDE, 4 * WIDE), BF16),
            pltpu.VMEM((WIDE, WIDE), BF16),
            pltpu.VMEM((WIDE, 4 * WIDE), BF16),
            pltpu.VMEM((4 * WIDE, WIDE), BF16),
            pltpu.VMEM((512, 128), F32),
            pltpu.VMEM((2, 16, 128), BF16),
            pltpu.VMEM((16, 16, 128), BF16),
            pltpu.VMEM((2, 8, 64, 512), BF16),
            pltpu.VMEM((4, 128, WIDE), BF16),
            pltpu.VMEM((4, 1, 128), jnp.int32),
            pltpu.VMEM((8, 16, 1, 128), jnp.int32),
            pltpu.VMEM((512, 128), F32),
            pltpu.VMEM((128, 128), F32),
            pltpu.VMEM((WIDE, 1024), BF16),
            pltpu.VMEM((WIDE, 512), BF16),
            pltpu.VMEM((512, 1024), F32),
            pltpu.VMEM((WIDE, 128), F32),
            pltpu.VMEM((WIDE, 128), F32),
            pltpu.VMEM((8, 16, WIDE), BF16),
            pltpu.VMEM((16, 8, WIDE), BF16),
            pltpu.VMEM((16, 8, WIDE), BF16),
            pltpu.VMEM((16, 8, WIDE), BF16),
            pltpu.VMEM((16, 8, WIDE), BF16),
            pltpu.VMEM((8, 16, WIDE), BF16),
            pltpu.VMEM((8, 16, WIDE), BF16),
            pltpu.VMEM((256, 128), F32),
            dma((13,)), dma, dma, dma, dma((4,)), dma, dma, dma, dma, dma, dma,
            dma, dma((2, 4, 2)), dma, dma, dma, dma, dma, dma, dma, dma, dma, dma,
        ],
        compiler_params=pltpu.CompilerParams(collective_id=0, has_side_effects=True),
    )(
        homolog_tensor.reshape(128, WIDE),
        pair_features.reshape(512, 128),
        entry_real_mask,
        chain_ids.reshape(4, 128),
        bias_proj.T,
        chain_bias,
        horizontal_matrices,
        horizontal_projector,
        column_proj,
        vertical_projector,
        expansion_matrix,
        contraction_matrix,
    )
    return updated.reshape(1, 128, WIDE)


def solution(mesh):
    torus = Mesh(
        mesh.devices.reshape(8, 2, 4, 2, mesh.shape["seq"]),
        ("dap_0", "dap_1", "dap_2", "dap_3", "seq"),
    )
    return jax.shard_map(
        body,
        mesh=torus,
        in_specs=(P(DAP, "seq", None), P("seq", DAP, None), P(DAP, "seq")) + (P(),) * 9,
        out_specs=P(DAP, "seq", None),
        check_vma=False,
    )
```

```python
import jax
import jax.numpy as jnp
from jax import lax
from jax.experimental import pallas as pl
from jax.experimental.pallas import tpu as pltpu
from jax.sharding import Mesh
from jax.sharding import PartitionSpec as P

HEADS = 8
DEPTH = 32
WIDE = 256
SCALE = DEPTH ** (-0.5)
EPS = 1e-05
DAP = ("dap_0", "dap_1", "dap_2", "dap_3")
MESH = pl.DeviceIdType.MESH
F32 = jnp.float32
BF16 = jnp.bfloat16


def layer_norm(x):
    center = x - jnp.mean(x, axis=-1, keepdims=True)
    spread = jnp.mean(center * center, axis=-1, keepdims=True)
    return center * lax.rsqrt(spread + EPS)


def mm(a, b):
    return jnp.dot(a, b, preferred_element_type=F32)


def far_id(g):
    return {"dap_0": lax.div(g, 2), "dap_1": lax.rem(g, 2)}


def near_id(q):
    return {"dap_2": lax.div(q, 2), "dap_3": lax.rem(q, 2)}


def kernel(
    hom_h, pair_h, mask_h, chain_h, bproj_h, cbias_h, wh_h, ph_h, wc_h, pv_h, ex_h, co_h,
    out,
    pair, chain, bproj, cbias, wh, ph, wc, pv, ex, co,
    xs, mine, zbuf, pack, biasall, homall, mrow, mzb, mcol, keep, keepc,
    qbd, vrow, vt, scores, ot, gt,
    a1s, a1, a2s, a2, b1s, b1, b2s, b2, fs,
    lsem, z_s, z_r, hom_s, hom_r, mrow_s, mrow_r, mp_s, mp_r, mz_s, mz_r,
    wave_s, wave_r, part_s, part_r, a1_s, a1_r, a2_s, a2_r, b1_s, b1_r, b2_s, b2_r,
):
    z = lax.axis_index("dap_0")
    y = lax.axis_index("dap_1")
    x = lax.axis_index("dap_2")
    c = lax.axis_index("dap_3")
    seq = lax.axis_index("seq")
    g = z * 2 + y
    q = x * 2 + c
    dap = g * 8 + q

    def local(n, src, dst):
        return pltpu.make_async_copy(src, dst, lsem.at[n])

    l_pair = local(0, pair_h, pair)
    l_chain = local(1, chain_h, chain)
    l_bproj = local(2, bproj_h, bproj)
    l_cbias = local(3, cbias_h, cbias)
    l_hom = local(4, hom_h, homall.at[seq])
    l_mrow = local(5, mask_h, mrow.at[seq])
    l_mcol = local(6, mask_h, mzb.at[g])
    l_wh = local(7, wh_h, wh)
    l_rest = [local(8 + n, a, b) for n, (a, b) in enumerate(
        ((ph_h, ph), (wc_h, wc), (pv_h, pv), (ex_h, ex), (co_h, co)))]
    for ld in (l_pair, l_chain, l_bproj, l_cbias, l_hom, l_mrow, l_mcol):
        ld.start()

    def remote(src, dst, ss, rs, device):
        return pltpu.make_async_remote_copy(
            src_ref=src, dst_ref=dst, send_sem=ss, recv_sem=rs, device_id=device,
            device_id_type=MESH)

    barrier = pltpu.get_barrier_semaphore()

    @pl.loop(1, 16)
    def _(p):
        pl.semaphore_signal(barrier, inc=1, device_id=far_id(lax.rem(g + p, 16)), device_id_type=MESH)

    @pl.loop(1, 4)
    def _(p):
        pl.semaphore_signal(barrier, inc=1, device_id={"seq": lax.rem(seq + p, 4)}, device_id_type=MESH)

    @pl.loop(1, 8)
    def _(p):
        pl.semaphore_signal(barrier, inc=1, device_id=near_id(lax.rem(q + p, 8)), device_id_type=MESH)

    l_wh.start()
    for ld in l_rest:
        ld.start()

    l_chain.wait()
    l_cbias.wait()
    diagonal = (lax.broadcasted_iota(jnp.int32, (8, 8), 0)
                == lax.broadcasted_iota(jnp.int32, (8, 8), 1))

    def by_head(row):
        return jnp.sum(jnp.where(diagonal, jnp.broadcast_to(row, (8, 8)), 0.0), axis=1, keepdims=True)

    cb0 = jnp.broadcast_to(by_head(cbias[0:1, :]), (8, 128))
    cb1 = jnp.broadcast_to(by_head(cbias[1:2, :]), (8, 128))
    row_chain = jnp.broadcast_to(chain[pl.ds(seq, 1), :], (8, 128))
    my_chain = jnp.broadcast_to(chain[pl.ds(lax.div(dap, 32), 1), :], (8, 128))
    lane = lax.broadcasted_iota(jnp.int32, (8, 128), 1) - lax.rem(dap, 32) * 4
    terms = []
    for j in range(4):
        own_chain = jnp.sum(jnp.where(lane == j, my_chain, 0).astype(F32), axis=1, keepdims=True)
        terms.append(jnp.where(row_chain.astype(F32) == own_chain, cb0, cb1))
    with jax.named_scope("waitpair"):
        l_pair.wait()
    xs[...] = layer_norm(pair[...].astype(F32))
    l_bproj.wait()
    parts = []
    for j in range(4):
        xj = xs[pl.ds(j, 128, stride=4), :]
        pj = lax.dot_general(bproj[...], xj, (((1,), (1,)), ((), ())), precision=lax.Precision.HIGHEST,
                             preferred_element_type=F32)
        parts.append(pj + terms[j])
    mine[...] = jnp.concatenate(parts, axis=0).astype(BF16)
    zbuf[g] = mine[...]
    l_hom.wait()
    l_mrow.wait()
    l_mcol.wait()
    qbd[...] = jnp.zeros_like(qbd)

    with jax.named_scope("barrier"):
        pl.semaphore_wait(barrier, 25)

    def z_copy(p):
        to = lax.rem(g + p, 16)
        return remote(mine, zbuf.at[g], z_s, z_r.at[lax.div(z, 4)], far_id(to))

    def hom_copy(p):
        to = lax.rem(seq + p, 4)
        return remote(homall.at[seq], homall.at[seq], hom_s, hom_r.at[seq], {"seq": to})

    def hom_recv(p):
        fr = lax.rem(seq + p, 4)
        return remote(homall.at[fr], homall.at[fr], hom_s, hom_r.at[fr], {"seq": fr})

    def mrow_copy(p):
        to = lax.rem(seq + p, 4)
        return remote(mrow.at[seq], mrow.at[seq], mrow_s, mrow_r, {"seq": to})

    def mz_copy(p):
        to = lax.rem(g + p, 16)
        return remote(mzb.at[g], mzb.at[g], mz_s, mz_r, far_id(to))

    def mp_copy(p):
        to = lax.rem(q + p, 8)
        return remote(mzb, mcol.at[q], mp_s, mp_r, near_id(to))

    def drain(ref, sem):
        pltpu.make_async_copy(ref, ref, sem).wait()

    pl.loop(1, 16)(lambda p: z_copy(p).start())
    pl.loop(1, 4)(lambda p: hom_copy(p).start())
    pl.loop(1, 16)(lambda p: mz_copy(p).start())
    pl.loop(1, 4)(lambda p: mrow_copy(p).start())

    def transposed(v):
        return v.astype(BF16).T

    def spread_queries(qt):
        for h in range(HEADS):
            qbd[h * 32:(h + 1) * 32, h * 128:(h + 1) * 128] = qt[h * 32:(h + 1) * 32, :]

    ri = lax.broadcasted_iota(jnp.int32, (128, 128), 0)
    ci = lax.broadcasted_iota(jnp.int32, (128, 128), 1)
    source = ((ri >> 3) & 1) * 64 + ((ri >> 2) & 1) * 32 + (ri >> 4) * 4 + (ri & 3)
    order = (ci == source).astype(BF16)

    def ordered(v):
        return mm(order, v).astype(BF16)

    def place(ref, b, v):
        rows = pl.ds(pl.multiple_of(lax.rem(b, 2) * 16, 16), 16)
        ref[lax.div(b, 2), :, rows, :] = v.reshape(8, 16, v.shape[-1])

    def block_scores(b, keys, values):
        place(scores, b, mm(keys.astype(BF16), qbd[...]))
        place(vrow, b, values)

    l_wh.wait()
    own = homall[seq].astype(F32)
    with jax.named_scope("ownqkv"):
        normed = layer_norm(own).astype(BF16)
        qg = mm(normed, wh[...])
        spread_queries(transposed(qg[:, :WIDE]))
        gt[...] = transposed(qg[:, 3 * WIDE:]).astype(F32)
        kv = mm(ordered(normed), wh[:, WIDE:3 * WIDE])
        block_scores(seq, kv[:, :WIDE], kv[:, WIDE:])

    def neighbour_block(p):
        b = lax.rem(seq + p, 4)
        with jax.named_scope(f"hom{p}"):
            hom_recv(p).wait_recv()
        kv = mm(ordered(layer_norm(homall[b].astype(F32)).astype(BF16)), wh[:, WIDE:3 * WIDE])
        block_scores(b, kv[:, :WIDE], kv[:, WIDE:])

    partner = {"dap_3": 1 - c}

    def wave_copy(e, p):
        to = lax.rem(q + p, 8)
        half = lax.rem(to, 2)
        return remote(pack.at[e, half], biasall.at[half, e, q], wave_s.at[e], wave_r.at[e], near_id(to))

    first = lax.div(z, 4)
    second = 1 - first

    def wave_send(e, count):
        with jax.named_scope(f"zwait{count}"):
            drain(zbuf.at[pl.ds(0, count)], z_r.at[e])
        xs[:256, :] = zbuf[pl.ds(e * 8, 8)].reshape(256, 128).astype(F32)
        for h in range(HEADS):
            pack[e, h // 4, :, (h % 4) * 128:(h % 4 + 1) * 128] = xs[pl.ds(h, 32, stride=8), :].astype(BF16)
        biasall[c, e, q] = pack[e, c]
        pl.loop(1, 8)(lambda p: wave_copy(e, p).start())

    def hand_over(e, n):
        with jax.named_scope(f"wave{n}"):
            drain(biasall.at[0, 0, pl.ds(0, 7)], wave_r.at[e])
        remote(biasall.at[c, e], biasall.at[c, e], part_s, part_r, partner).start()

    wave_send(first, 7)
    wave_send(second, 8)
    with jax.named_scope("nb1"):
        neighbour_block(1)
    with jax.named_scope("nb3"):
        neighbour_block(3)
    hand_over(first, 0)
    with jax.named_scope("nb2"):
        neighbour_block(2)
    with jax.named_scope("mask"):
        vt[...] = vrow[...].reshape(512, WIDE).astype(BF16).T
        drain(mrow.at[pl.ds(0, 3)], mrow_r)
        for b in range(4):
            place(keep, b, mm(order, jnp.broadcast_to(mrow[b].astype(F32), (128, 128)).T.astype(BF16)))
        drain(mzb.at[pl.ds(0, 15)], mz_r)
    pl.loop(1, 8)(lambda p: mp_copy(p).start())
    mcol[q] = mzb[...]
    hand_over(second, 1)

    def softmax_out(s, vth):
        m = jnp.max(s, axis=0, keepdims=True)
        e = jnp.exp(s - m)
        w = (e * (1.0 / jnp.sum(e, axis=0, keepdims=True))).astype(BF16)
        return mm(vth, w)

    def row_head(half, h):
        head = half * 4 + h
        lanes = pl.ds(pl.multiple_of(head * 128, 128), 128)
        rows = pl.ds(pl.multiple_of(head * 32, 32), 32)
        s = scores[:, :, :, lanes].reshape(512, 128) * SCALE
        s = s + biasall[half, :, :, :, h * 128:(h + 1) * 128].reshape(512, 128).astype(F32)
        s = jnp.where(keep[...].reshape(512, 128) > 0.0, s, -1000000000.0)
        ot[rows, :] = softmax_out(s, vt[rows, :])

    with jax.named_scope("rowattn"):
        for h in range(4):
            row_head(c, h)
    with jax.named_scope("partner"):
        drain(biasall.at[1 - c], part_r)
    with jax.named_scope("rowattn2"):
        for h in range(4):
            row_head(1 - c, h)

    def split(v):
        fs[:128, :] = v[:, :128].astype(F32)
        fs[128:, :] = v[:, 128:].astype(F32)

    def gated_project(w):
        g = (jax.nn.sigmoid(gt[...]) * ot[...]).astype(BF16)
        return mm(g.T, w)

    with jax.named_scope("rowproj"):
        l_rest[0].wait()
        one = (homall[seq].astype(F32) + gated_project(ph[...])).astype(BF16).astype(F32)
        a1s[...] = one.reshape(16, 8, WIDE).astype(BF16)
        a1[g] = a1s[g]

    def a1_copy(p):
        to = lax.rem(g + p, 16)
        return remote(a1s.at[to], a1.at[g], a1_s, a1_r, far_id(to))

    pl.loop(1, 16)(lambda p: a1_copy(p).start())
    with jax.named_scope("waita1"):
        drain(a1.at[pl.ds(0, 15)], a1_r)

    split(a1[...].astype(F32).reshape(128, WIDE))
    for n in range(8):
        for t in range(2):
            a2s[n, :, t * 128:(t + 1) * 128] = fs[pl.ds(t * 128 + n, 16, stride=8), :].astype(BF16)
    a2[q] = a2s[q]

    def a2_copy(p):
        to = lax.rem(q + p, 8)
        return remote(a2s.at[to], a2.at[q], a2_s, a2_r, near_id(to))

    pl.loop(1, 8)(lambda p: a2_copy(p).start())
    for ld in l_rest[1:]:
        ld.wait()
    with jax.named_scope("keepc"):
        drain(mcol.at[pl.ds(0, 7)], mp_r)
        pick = (ri == dap).astype(BF16)
        keepc[...] = mm(mcol[...].reshape(128, 128).astype(F32).astype(BF16), pick)
    with jax.named_scope("waita2"):
        drain(a2.at[pl.ds(0, 7)], a2_r)

    with jax.named_scope("colattn"):
        col = a2[...].reshape(128, WIDE).astype(F32)
        qkvg = mm(layer_norm(col).astype(BF16), wc[...])
        spread_queries(transposed(qkvg[:, :WIDE]))
        gt[...] = transposed(qkvg[:, 3 * WIDE:]).astype(F32)
        cs = mm(qkvg[:, WIDE:2 * WIDE].astype(BF16), qbd[...]) * SCALE
        cvt = transposed(qkvg[:, 2 * WIDE:3 * WIDE])
        for h in range(HEADS):
            s = jnp.where(keepc[...] > 0.0, cs[:, h * 128:(h + 1) * 128], -1000000000.0)
            ot[h * 32:(h + 1) * 32, :] = softmax_out(s, cvt[h * 32:(h + 1) * 32, :])
    with jax.named_scope("transition"):
        two = col + gated_project(pv[...])
        inner = jnp.maximum(mm(layer_norm(two).astype(BF16), ex[...]), 0.0).astype(BF16)
        done = two + mm(inner, co[...])
        b1s[...] = done.astype(BF16).reshape(8, 16, WIDE)
        b1[q] = b1s[q]

    def b1_copy(p):
        to = lax.rem(q + p, 8)
        return remote(b1s.at[to], b1.at[q], b1_s, b1_r, near_id(to))

    pl.loop(1, 8)(lambda p: b1_copy(p).start())
    with jax.named_scope("waitb1"):
        drain(b1.at[pl.ds(0, 7)], b1_r)
    split(b1[...].reshape(128, WIDE))
    for n in range(16):
        for t in range(2):
            b2s[n, :, t * 128:(t + 1) * 128] = fs[pl.ds(t * 128 + n, 8, stride=16), :].astype(BF16)
    b2[g] = b2s[g]

    def b2_copy(p):
        to = lax.rem(g + p, 16)
        return remote(b2s.at[to], b2.at[g], b2_s, b2_r, far_id(to))

    pl.loop(1, 16)(lambda p: b2_copy(p).start())

    drain(zbuf.at[pl.ds(0, 15)], z_s)
    for e in range(2):
        drain(biasall.at[0, 0, pl.ds(0, 7)], wave_s.at[e])
    drain(mcol.at[pl.ds(0, 7)], mp_s)
    drain(a1.at[pl.ds(0, 15)], a1_s)
    drain(a2.at[pl.ds(0, 7)], a2_s)
    drain(b1.at[pl.ds(0, 7)], b1_s)
    drain(mzb.at[pl.ds(0, 15)], mz_s)
    drain(homall.at[pl.ds(0, 3)], hom_s)
    drain(mrow.at[pl.ds(0, 3)], mrow_s)
    drain(biasall.at[0], part_s)
    with jax.named_scope("waitb2"):
        drain(b2.at[pl.ds(0, 15)], b2_r)
    drain(b2.at[pl.ds(0, 15)], b2_s)
    out[...] = b2[...].astype(F32).reshape(128, WIDE).astype(BF16)


def body(
    homolog_tensor, pair_features, entry_real_mask, chain_ids, horizontal_matrices,
    horizontal_projector, bias_proj, chain_bias, column_proj, vertical_projector,
    expansion_matrix, contraction_matrix,
):
    vmem = pl.BlockSpec(memory_space=pltpu.VMEM)
    hbm = pl.BlockSpec(memory_space=pl.ANY)
    dma = pltpu.SemaphoreType.DMA
    updated = pl.pallas_call(
        kernel,
        name="msa_block",
        out_shape=pltpu.VMEM((128, WIDE), BF16),
        in_specs=[hbm] * 12,
        out_specs=vmem,
        scratch_shapes=[
            pltpu.VMEM((512, 128), BF16),
            pltpu.VMEM((4, 128), jnp.int32),
            pltpu.VMEM((8, 128), F32),
            pltpu.VMEM((2, 8), F32),
            pltpu.VMEM((WIDE, 4 * WIDE), BF16),
            pltpu.VMEM((WIDE, WIDE), BF16),
            pltpu.VMEM((WIDE, 4 * WIDE), BF16),
            pltpu.VMEM((WIDE, WIDE), BF16),
            pltpu.VMEM((WIDE, 4 * WIDE), BF16),
            pltpu.VMEM((4 * WIDE, WIDE), BF16),
            pltpu.VMEM((512, 128), F32),
            pltpu.VMEM((32, 128), BF16),
            pltpu.VMEM((16, 32, 128), BF16),
            pltpu.VMEM((2, 2, 32, 512), BF16),
            pltpu.VMEM((2, 2, 8, 32, 512), BF16),
            pltpu.VMEM((4, 128, WIDE), BF16),
            pltpu.VMEM((4, 1, 128), jnp.int32),
            pltpu.VMEM((16, 1, 128), jnp.int32),
            pltpu.VMEM((8, 16, 1, 128), jnp.int32),
            pltpu.VMEM((2, 8, 32, 128), F32),
            pltpu.VMEM((128, 128), F32),
            pltpu.VMEM((WIDE, 1024), BF16),
            pltpu.VMEM((2, 8, 32, WIDE), F32),
            pltpu.VMEM((WIDE, 512), BF16),
            pltpu.VMEM((2, 8, 32, 1024), F32),
            pltpu.VMEM((WIDE, 128), F32),
            pltpu.VMEM((WIDE, 128), F32),
            pltpu.VMEM((16, 8, WIDE), BF16),
            pltpu.VMEM((16, 8, WIDE), BF16),
            pltpu.VMEM((8, 16, WIDE), BF16),
            pltpu.VMEM((8, 16, WIDE), BF16),
            pltpu.VMEM((8, 16, WIDE), BF16),
            pltpu.VMEM((8, 16, WIDE), BF16),
            pltpu.VMEM((16, 8, WIDE), BF16),
            pltpu.VMEM((16, 8, WIDE), BF16),
            pltpu.VMEM((256, 128), F32),
            dma((13,)), dma, dma((2,)), dma, dma((4,)), dma, dma, dma, dma, dma, dma,
            dma((2,)), dma((2,)), dma, dma, dma, dma, dma, dma, dma, dma, dma, dma,
        ],
        compiler_params=pltpu.CompilerParams(collective_id=0, has_side_effects=True),
    )(
        homolog_tensor.reshape(128, WIDE),
        pair_features.reshape(512, 128),
        entry_real_mask,
        chain_ids.reshape(4, 128),
        bias_proj.T,
        chain_bias,
        horizontal_matrices,
        horizontal_projector,
        column_proj,
        vertical_projector,
        expansion_matrix,
        contraction_matrix,
    )
    return updated.reshape(1, 128, WIDE)


def solution(mesh):
    torus = Mesh(
        mesh.devices.reshape(8, 2, 4, 2, mesh.shape["seq"]),
        ("dap_0", "dap_1", "dap_2", "dap_3", "seq"),
    )
    return jax.shard_map(
        body,
        mesh=torus,
        in_specs=(P(DAP, "seq", None), P("seq", DAP, None), P(DAP, "seq")) + (P(),) * 9,
        out_specs=P(DAP, "seq", None),
        check_vma=False,
    )
```

```python
import jax
import jax.numpy as jnp
from jax import lax
from jax.experimental import pallas as pl
from jax.experimental.pallas import tpu as pltpu
from jax.sharding import Mesh
from jax.sharding import PartitionSpec as P

HEADS = 8
DEPTH = 32
WIDE = 256
SCALE = DEPTH ** (-0.5)
EPS = 1e-05
DAP = ("dap_0", "dap_1", "dap_2", "dap_3")
MESH = pl.DeviceIdType.MESH
F32 = jnp.float32
BF16 = jnp.bfloat16


def layer_norm(x):
    center = x - jnp.mean(x, axis=-1, keepdims=True)
    spread = jnp.mean(center * center, axis=-1, keepdims=True)
    return center * lax.rsqrt(spread + EPS)


def mm(a, b):
    return jnp.dot(a, b, preferred_element_type=F32)


FAR = tuple((dz, dy) for dz in (4, 3, 5, 2, 6, 1, 7, 0) for dy in (1, 0) if dz or dy)
HALVES = tuple((o, i, dy) for o in range(2) for i in (1, 3, 2, 0) for dy in range(2) if o or i or dy)
ALL = tuple((dx, dy, dc) for dx in (2, 1, 3, 0) for dy in (1, 0) for dc in (1, 0))
NEAR = tuple((dx, dc) for dx in (2, 1, 3, 0) for dc in (1, 0) if dx or dc)


def kernel(
    hom_h, pair_h, mask_h, chain_h, bproj_h, cbias_h, wh_h, ph_h, wc_h, pv_h, ex_h, co_h,
    out,
    pair, chain, bproj, cbias, wh, ph, wc, pv, ex, co,
    xs, mine, zbuf, pack, biasall, homall, mrow, mzb, mcol, keepc,
    qbd, vrow, vt, scores, ot, gt,
    a1s, a1, b1s, b2, fs,
    lsem, z_s, z_r, hom_s, hom_r, mrow_s, mrow_r, mp_s, mp_r, mz_s, mz_r,
    wave_s, wave_r, part_s, part_r, a1_s, a1_r, b2_s, b2_r,
):
    z = lax.axis_index("dap_0")
    y = lax.axis_index("dap_1")
    x = lax.axis_index("dap_2")
    c = lax.axis_index("dap_3")
    seq = lax.axis_index("seq")
    g = z * 2 + y
    q = x * 2 + c
    dap = g * 8 + q

    def local(n, src, dst):
        return pltpu.make_async_copy(src, dst, lsem.at[n])

    l_pair = local(0, pair_h, pair)
    l_chain = local(1, chain_h, chain)
    l_bproj = local(2, bproj_h, bproj)
    l_cbias = local(3, cbias_h, cbias)
    l_hom = local(4, hom_h, homall.at[seq])
    l_mrow = local(5, mask_h, mrow.at[seq])
    l_mcol = local(6, mask_h, mzb.at[g])
    l_wh = local(7, wh_h, wh)
    l_rest = [local(8 + n, a, b) for n, (a, b) in enumerate(
        ((ph_h, ph), (wc_h, wc), (pv_h, pv), (ex_h, ex), (co_h, co)))]
    for ld in (l_pair, l_chain, l_cbias, l_bproj):
        ld.start()

    def remote(src, dst, ss, rs, device):
        return pltpu.make_async_remote_copy(
            src_ref=src, dst_ref=dst, send_sem=ss, recv_sem=rs, device_id=device,
            device_id_type=MESH)

    barrier = pltpu.get_barrier_semaphore()

    def far(n):
        zz, yy = lax.rem(z + n[0], 8), lax.rem(y + n[1], 2)
        return zz * 2 + yy, {"dap_0": zz, "dap_1": yy}

    def near(n):
        xx, cc = lax.rem(x + n[0], 4), lax.rem(c + n[1], 2)
        return xx * 2 + cc, {"dap_2": xx, "dap_3": cc}

    with jax.named_scope("signals"):
        for n in FAR:
            pl.semaphore_signal(barrier, inc=1, device_id=far(n)[1], device_id_type=MESH)
        for n in (2, 1, 3):
            pl.semaphore_signal(barrier, inc=1, device_id={"seq": lax.rem(seq + n, 4)}, device_id_type=MESH)
        for n in NEAR:
            pl.semaphore_signal(barrier, inc=1, device_id=near(n)[1], device_id_type=MESH)

    for ld in (l_hom, l_mrow, l_mcol):
        ld.start()
    l_wh.start()
    for ld in l_rest:
        ld.start()

    l_chain.wait()
    l_cbias.wait()
    diagonal = (lax.broadcasted_iota(jnp.int32, (8, 8), 0)
                == lax.broadcasted_iota(jnp.int32, (8, 8), 1))

    def by_head(row):
        return jnp.sum(jnp.where(diagonal, jnp.broadcast_to(row, (8, 8)), 0.0), axis=1, keepdims=True)

    cb0 = jnp.broadcast_to(by_head(cbias[0:1, :]), (8, 128))
    cb1 = jnp.broadcast_to(by_head(cbias[1:2, :]), (8, 128))
    row_chain = jnp.broadcast_to(chain[pl.ds(seq, 1), :], (8, 128))
    my_chain = jnp.broadcast_to(chain[pl.ds(lax.div(dap, 32), 1), :], (8, 128))
    lane = lax.broadcasted_iota(jnp.int32, (8, 128), 1) - lax.rem(dap, 32) * 4
    terms = []
    for j in range(4):
        own_chain = jnp.sum(jnp.where(lane == j, my_chain, 0).astype(F32), axis=1, keepdims=True)
        terms.append(jnp.where(row_chain.astype(F32) == own_chain, cb0, cb1))
    with jax.named_scope("waitpair"):
        l_pair.wait()
    xs[...] = layer_norm(pair[...].astype(F32))
    l_bproj.wait()
    w_top = bproj[...].astype(BF16).astype(F32)
    w_both = jnp.concatenate([w_top, bproj[...] - w_top], axis=0).astype(BF16)

    def across(v):
        return lax.dot_general(w_both, v, (((1,), (1,)), ((), ())), preferred_element_type=F32)

    parts = []
    for j in range(4):
        xj = xs[pl.ds(j, 128, stride=4), :]
        top = xj.astype(BF16)
        rest = (xj - top.astype(F32)).astype(BF16)
        pj = across(top) + across(rest)
        parts.append(pj[:8] + pj[8:] + terms[j])
    mine[...] = jnp.concatenate(parts, axis=0).astype(BF16)
    zbuf[g] = mine[...]
    l_hom.wait()
    l_mrow.wait()
    l_mcol.wait()
    qbd[...] = jnp.zeros_like(qbd)

    with jax.named_scope("barrier"):
        pl.semaphore_wait(barrier, 25)

    def z_copy(n):
        zz = lax.rem(lax.div(z, 4) + n[0], 2) * 4 + lax.rem(z + n[1], 4)
        device = {"dap_0": zz, "dap_1": lax.rem(y + n[2], 2)}
        return remote(mine, zbuf.at[g], z_s, z_r.at[lax.div(z, 4)], device)

    def hom_copy(p):
        to = lax.rem(seq + p, 4)
        return remote(homall.at[seq], homall.at[seq], hom_s, hom_r.at[seq], {"seq": to})

    def hom_recv(p):
        fr = lax.rem(seq + p, 4)
        return remote(homall.at[fr], homall.at[fr], hom_s, hom_r.at[fr], {"seq": fr})

    def mrow_copy(p):
        to = lax.rem(seq + p, 4)
        return remote(mrow.at[seq], mrow.at[seq], mrow_s, mrow_r, {"seq": to})

    def mz_copy(n):
        to, device = far(n)
        return remote(mzb.at[g], mzb.at[g], mz_s, mz_r, device)

    def mp_copy(n):
        to, device = near(n)
        return remote(mzb, mcol.at[q], mp_s, mp_r, device)

    def drain(ref, sem):
        pltpu.make_async_copy(ref, ref, sem).wait()

    for n in HALVES:
        z_copy(n).start()
    for p in (2, 1, 3):
        mrow_copy(p).start()
    for p in (2, 1, 3):
        hom_copy(p).start()
    for n in FAR:
        mz_copy(n).start()

    def transposed(v):
        return v.astype(BF16).T

    def spread_queries(qt):
        for h in range(HEADS):
            qbd[h * 32:(h + 1) * 32, h * 128:(h + 1) * 128] = qt[h * 32:(h + 1) * 32, :]

    ri = lax.broadcasted_iota(jnp.int32, (128, 128), 0)
    ci = lax.broadcasted_iota(jnp.int32, (128, 128), 1)
    source = ((ri >> 3) & 1) * 64 + ((ri >> 2) & 1) * 32 + (ri >> 4) * 4 + (ri & 3)
    order = (ci == source).astype(BF16)

    def ordered(v):
        return mm(order, v).astype(BF16)

    def place(ref, b, v):
        rows = pl.ds(pl.multiple_of(lax.rem(b, 2) * 16, 16), 16)
        ref[lax.div(b, 2), :, rows, :] = v.reshape(8, 16, v.shape[-1])

    def block_scores(b, s, values):
        seen = mm(order, jnp.broadcast_to(mrow[b].astype(F32), (128, 128)).T.astype(BF16)) > 0.0
        s = [jnp.where(seen, s[:, h * 128:(h + 1) * 128] * SCALE, -1e30) for h in range(HEADS)]
        place(scores, b, jnp.concatenate(s, axis=1))
        place(vrow, b, values)

    l_wh.wait()
    own = homall[seq].astype(F32)
    with jax.named_scope("ownqkv"):
        normed = layer_norm(own).astype(BF16)
        qg = mm(normed, wh[...])
        spread_queries(transposed(qg[:, :WIDE]))
        gt[...] = transposed(qg[:, 3 * WIDE:]).astype(F32)
        kv = mm(ordered(normed), wh[:, WIDE:3 * WIDE])
        block_scores(seq, mm(kv[:, :WIDE].astype(BF16), qbd[...]), kv[:, WIDE:])

    def neighbour_blocks():
        drain(mrow.at[pl.ds(0, 3)], mrow_r)
        blocks = [lax.rem(seq + p, 4) for p in (1, 3, 2)]
        for p in (1, 3, 2):
            with jax.named_scope(f"hom{p}"):
                hom_recv(p).wait_recv()
        with jax.named_scope("nb"):
            normed = [ordered(layer_norm(homall[b].astype(F32)).astype(BF16)) for b in blocks]
            kv = mm(jnp.concatenate(normed, axis=0), wh[:, WIDE:3 * WIDE])
            s = mm(kv[:, :WIDE].astype(BF16), qbd[...])
            for n, b in enumerate(blocks):
                block_scores(b, s[n * 128:(n + 1) * 128], kv[n * 128:(n + 1) * 128, WIDE:])
            vt[...] = vrow[...].reshape(512, WIDE).astype(BF16).T

    partner = {"dap_3": 1 - c}

    def wave_copy(e, n):
        to, device = near(n)
        half = device["dap_3"]
        return remote(pack.at[e, half], biasall.at[half, e, q], wave_s.at[e], wave_r.at[e], device)

    first = lax.div(z, 4)
    second = 1 - first

    def wave_send(e, count):
        with jax.named_scope(f"zwait{count}"):
            drain(zbuf.at[pl.ds(0, count)], z_r.at[e])
        xs[:256, :] = zbuf[pl.ds(e * 8, 8)].reshape(256, 128).astype(F32)
        for h in range(HEADS):
            pack[e, h // 4, :, (h % 4) * 128:(h % 4 + 1) * 128] = xs[pl.ds(h, 32, stride=8), :].astype(BF16)
        biasall[c, e, q] = pack[e, c]
        for n in NEAR:
            wave_copy(e, n).start()

    def hand_over(e, n):
        with jax.named_scope(f"wave{n}"):
            drain(biasall.at[0, 0, pl.ds(0, 7)], wave_r.at[e])
        remote(biasall.at[c, e], biasall.at[c, e], part_s, part_r, partner).start()

    wave_send(first, 7)
    wave_send(second, 8)
    hand_over(first, 0)
    neighbour_blocks()
    hand_over(second, 1)

    def softmax_out(s, vth):
        m = jnp.max(s, axis=0, keepdims=True)
        e = jnp.exp(s - m)
        w = (e * (1.0 / jnp.sum(e, axis=0, keepdims=True))).astype(BF16)
        return mm(vth, w)

    def row_head(half, h):
        head = half * 4 + h
        lanes = pl.ds(pl.multiple_of(head * 128, 128), 128)
        rows = pl.ds(pl.multiple_of(head * 32, 32), 32)
        s = scores[:, :, :, lanes].reshape(512, 128)
        s = s + biasall[half, :, :, :, h * 128:(h + 1) * 128].reshape(512, 128).astype(F32)
        ot[rows, :] = softmax_out(s, vt[rows, :])

    with jax.named_scope("rowattn"):
        for h in range(4):
            row_head(c, h)
    with jax.named_scope("partner"):
        drain(biasall.at[1 - c], part_r)
    with jax.named_scope("rowattn2"):
        for h in range(4):
            row_head(1 - c, h)

    def pairs(v):
        fs[pl.ds(0, 128, stride=2), :] = v[:, :128]
        fs[pl.ds(1, 128, stride=2), :] = v[:, 128:]
        return fs[...].astype(BF16).reshape(128, 2, 128)

    def unpaired(v):
        fs[...] = v.reshape(256, 128).astype(F32)
        return jnp.concatenate([fs[pl.ds(0, 128, stride=2), :], fs[pl.ds(1, 128, stride=2), :]], axis=1)

    mine_row = q * 16 + g

    def exchange(copy):
        def rest(dz, dims):
            for dx, dy, dc in dims:
                to_g = lax.rem(z + dz, 8) * 2 + lax.rem(y + dy, 2)
                to_q = lax.rem(x + dx, 4) * 2 + lax.rem(c + dc, 2)
                copy(to_g, to_q, {
                    "dap_0": lax.rem(z + dz, 8), "dap_1": lax.rem(y + dy, 2),
                    "dap_2": lax.rem(x + dx, 4), "dap_3": lax.rem(c + dc, 2)}).start()

        @pl.loop(0, 7)
        def _(n):
            rest(4 + lax.div(n + 1, 2) * (1 - 2 * lax.rem(n, 2)), ALL)

        rest(0, ALL[:-1])

    def gated_project(w):
        g = (jax.nn.sigmoid(gt[...]) * ot[...]).astype(BF16)
        return mm(g.T, w)

    with jax.named_scope("rowproj"):
        l_rest[0].wait()
        one = homall[seq].astype(F32) + gated_project(ph[...])
        a1s[...] = pairs(one)
        a1[mine_row] = a1s[dap]

    def a1_copy(to_g, to_q, device):
        return remote(a1s.at[to_g * 8 + to_q], a1.at[mine_row], a1_s, a1_r, device)

    exchange(a1_copy)
    drain(mzb.at[pl.ds(0, 15)], mz_r)
    for n in NEAR:
        mp_copy(n).start()
    mcol[q] = mzb[...]
    for ld in l_rest[1:]:
        ld.wait()
    with jax.named_scope("keepc"):
        drain(mcol.at[pl.ds(0, 7)], mp_r)
        pick = (ri == dap).astype(BF16)
        keepc[...] = mm(mcol[...].reshape(128, 128).astype(F32).astype(BF16), pick)
    with jax.named_scope("waita1"):
        drain(a1.at[pl.ds(0, 127)], a1_r)

    with jax.named_scope("colattn"):
        col = unpaired(a1[...])
        qkvg = mm(layer_norm(col).astype(BF16), wc[...])
        spread_queries(transposed(qkvg[:, :WIDE]))
        gt[...] = transposed(qkvg[:, 3 * WIDE:]).astype(F32)
        cs = mm(qkvg[:, WIDE:2 * WIDE].astype(BF16), qbd[...]) * SCALE
        cvt = transposed(qkvg[:, 2 * WIDE:3 * WIDE])
        for h in range(HEADS):
            s = jnp.where(keepc[...] > 0.0, cs[:, h * 128:(h + 1) * 128], -1000000000.0)
            ot[h * 32:(h + 1) * 32, :] = softmax_out(s, cvt[h * 32:(h + 1) * 32, :])
    with jax.named_scope("transition"):
        two = col + gated_project(pv[...])
        inner = jnp.maximum(mm(layer_norm(two).astype(BF16), ex[...]), 0.0).astype(BF16)
        done = two + mm(inner, co[...])
        b1s[...] = pairs(done)
        b2[dap] = b1s[mine_row]

    def b2_copy(to_g, to_q, device):
        return remote(b1s.at[to_q * 16 + to_g], b2.at[dap], b2_s, b2_r, device)

    exchange(b2_copy)

    drain(zbuf.at[pl.ds(0, 15)], z_s)
    for e in range(2):
        drain(biasall.at[0, 0, pl.ds(0, 7)], wave_s.at[e])
    drain(mcol.at[pl.ds(0, 7)], mp_s)
    drain(a1.at[pl.ds(0, 127)], a1_s)
    drain(mzb.at[pl.ds(0, 15)], mz_s)
    drain(homall.at[pl.ds(0, 3)], hom_s)
    drain(mrow.at[pl.ds(0, 3)], mrow_s)
    drain(biasall.at[0], part_s)
    with jax.named_scope("waitb2"):
        drain(b2.at[pl.ds(0, 127)], b2_r)
    drain(b2.at[pl.ds(0, 127)], b2_s)
    out[...] = unpaired(b2[...]).astype(BF16)


def body(
    homolog_tensor, pair_features, entry_real_mask, chain_ids, horizontal_matrices,
    horizontal_projector, bias_proj, chain_bias, column_proj, vertical_projector,
    expansion_matrix, contraction_matrix,
):
    vmem = pl.BlockSpec(memory_space=pltpu.VMEM)
    hbm = pl.BlockSpec(memory_space=pl.ANY)
    dma = pltpu.SemaphoreType.DMA
    updated = pl.pallas_call(
        kernel,
        name="msa_block",
        out_shape=pltpu.VMEM((128, WIDE), BF16),
        in_specs=[hbm] * 12,
        out_specs=vmem,
        scratch_shapes=[
            pltpu.VMEM((512, 128), BF16),
            pltpu.VMEM((4, 128), jnp.int32),
            pltpu.VMEM((8, 128), F32),
            pltpu.VMEM((2, 8), F32),
            pltpu.VMEM((WIDE, 4 * WIDE), BF16),
            pltpu.VMEM((WIDE, WIDE), BF16),
            pltpu.VMEM((WIDE, 4 * WIDE), BF16),
            pltpu.VMEM((WIDE, WIDE), BF16),
            pltpu.VMEM((WIDE, 4 * WIDE), BF16),
            pltpu.VMEM((4 * WIDE, WIDE), BF16),
            pltpu.VMEM((512, 128), F32),
            pltpu.VMEM((32, 128), BF16),
            pltpu.VMEM((16, 32, 128), BF16),
            pltpu.VMEM((2, 2, 32, 512), BF16),
            pltpu.VMEM((2, 2, 8, 32, 512), BF16),
            pltpu.VMEM((4, 128, WIDE), BF16),
            pltpu.VMEM((4, 1, 128), jnp.int32),
            pltpu.VMEM((16, 1, 128), jnp.int32),
            pltpu.VMEM((8, 16, 1, 128), jnp.int32),
            pltpu.VMEM((128, 128), F32),
            pltpu.VMEM((WIDE, 1024), BF16),
            pltpu.VMEM((2, 8, 32, WIDE), F32),
            pltpu.VMEM((WIDE, 512), BF16),
            pltpu.VMEM((2, 8, 32, 1024), F32),
            pltpu.VMEM((WIDE, 128), F32),
            pltpu.VMEM((WIDE, 128), F32),
            pltpu.VMEM((128, 2, 128), BF16),
            pltpu.VMEM((128, 2, 128), BF16),
            pltpu.VMEM((128, 2, 128), BF16),
            pltpu.VMEM((128, 2, 128), BF16),
            pltpu.VMEM((256, 128), F32),
            dma((13,)), dma, dma((2,)), dma, dma((4,)), dma, dma, dma, dma, dma, dma,
            dma((2,)), dma((2,)), dma, dma, dma, dma, dma, dma,
        ],
        compiler_params=pltpu.CompilerParams(collective_id=0, has_side_effects=True),
    )(
        homolog_tensor.reshape(128, WIDE),
        pair_features.reshape(512, 128),
        entry_real_mask,
        chain_ids.reshape(4, 128),
        bias_proj.T,
        chain_bias,
        horizontal_matrices,
        horizontal_projector,
        column_proj,
        vertical_projector,
        expansion_matrix,
        contraction_matrix,
    )
    return updated.reshape(1, 128, WIDE)


def solution(mesh):
    torus = Mesh(
        mesh.devices.reshape(8, 2, 4, 2, mesh.shape["seq"]),
        ("dap_0", "dap_1", "dap_2", "dap_3", "seq"),
    )
    return jax.shard_map(
        body,
        mesh=torus,
        in_specs=(P(DAP, "seq", None), P("seq", DAP, None), P(DAP, "seq")) + (P(),) * 9,
        out_specs=P(DAP, "seq", None),
        check_vma=False,
    )
```

```python
import jax
import jax.numpy as jnp
from jax import lax
from jax.experimental import pallas as pl
from jax.experimental.pallas import tpu as pltpu
from jax.sharding import Mesh
from jax.sharding import PartitionSpec as P

HEADS = 8
DEPTH = 32
WIDE = 256
SCALE = DEPTH ** (-0.5)
EPS = 1e-05
DAP = ("dap_0", "dap_1", "dap_2", "dap_3")
MESH = pl.DeviceIdType.MESH
F32 = jnp.float32
BF16 = jnp.bfloat16


def layer_norm(x):
    center = x - jnp.mean(x, axis=-1, keepdims=True)
    spread = jnp.mean(center * center, axis=-1, keepdims=True)
    return center * lax.rsqrt(spread + EPS)


def mm(a, b):
    return jnp.dot(a, b, preferred_element_type=F32)


FAR = tuple((dz, dy) for dz in (4, 3, 5, 2, 6, 1, 7, 0) for dy in (1, 0) if dz or dy)
HALVES = tuple((o, i, dy) for o in range(2) for i in (1, 3, 2, 0) for dy in range(2) if o or i or dy)
WAVE = tuple((dx, core) for core in range(2) for dx in (2, 1, 3)) + ((0, 0),)
ALL = tuple((dx, dy, dc) for dx in (2, 1, 3, 0) for dy in (1, 0) for dc in (1, 0))
NEAR = tuple((dx, dc) for dx in (2, 1, 3, 0) for dc in (1, 0) if dx or dc)


def kernel(
    hom_h, pair_h, mask_h, chain_h, bproj_h, cbias_h, wh_h, ph_h, wc_h, pv_h, ex_h, co_h,
    out,
    pair, chain, bproj, cbias, wh, ph, wc, pv, ex, co,
    xs, mine, zbuf, pack, biasall, homall, mrow, mzb, mcol, keepc,
    qbd, vrow, vt, scores, top, total, ot, gt,
    a1s, a1, b1s, b2, fs,
    lsem, z_s, z_r, hom_s, hom_r, mrow_s, mrow_r, mp_s, mp_r, mz_s, mz_r,
    wave_s, wave_r, part_s, part_r, a1_s, a1_r, b2_s, b2_r,
):
    z = lax.axis_index("dap_0")
    y = lax.axis_index("dap_1")
    x = lax.axis_index("dap_2")
    c = lax.axis_index("dap_3")
    seq = lax.axis_index("seq")
    g = z * 2 + y
    q = x * 2 + c
    dap = g * 8 + q

    def local(n, src, dst):
        return pltpu.make_async_copy(src, dst, lsem.at[n])

    l_pair = local(0, pair_h, pair)
    l_chain = local(1, chain_h, chain)
    l_bproj = local(2, bproj_h, bproj)
    l_cbias = local(3, cbias_h, cbias)
    l_hom = local(4, hom_h, homall.at[seq])
    l_mrow = local(5, mask_h, mrow.at[seq])
    l_mcol = local(6, mask_h, mzb.at[g])
    l_wh = local(7, wh_h, wh)
    l_rest = [local(8 + n, a, b) for n, (a, b) in enumerate(
        ((ph_h, ph), (wc_h, wc), (pv_h, pv), (ex_h, ex), (co_h, co)))]
    with jax.named_scope("start"):
        for ld in (l_pair, l_chain, l_cbias, l_bproj):
            ld.start()

    def remote(src, dst, ss, rs, device):
        return pltpu.make_async_remote_copy(
            src_ref=src, dst_ref=dst, send_sem=ss, recv_sem=rs, device_id=device,
            device_id_type=MESH)

    barrier = pltpu.get_barrier_semaphore()

    def far(n):
        zz, yy = lax.rem(z + n[0], 8), lax.rem(y + n[1], 2)
        return zz * 2 + yy, {"dap_0": zz, "dap_1": yy}

    def near(n):
        xx, cc = lax.rem(x + n[0], 4), lax.rem(c + n[1], 2)
        return xx * 2 + cc, {"dap_2": xx, "dap_3": cc}

    with jax.named_scope("signals"):
        for n in FAR:
            pl.semaphore_signal(barrier, inc=1, device_id=far(n)[1], device_id_type=MESH)
        for n in (2, 1, 3):
            pl.semaphore_signal(barrier, inc=1, device_id={"seq": lax.rem(seq + n, 4)}, device_id_type=MESH)
        for n in NEAR:
            pl.semaphore_signal(barrier, inc=1, device_id=near(n)[1], device_id_type=MESH)

    for ld in (l_hom, l_mrow, l_mcol):
        ld.start()
    l_wh.start()
    for ld in l_rest:
        ld.start()

    l_chain.wait()
    l_cbias.wait()
    diagonal = (lax.broadcasted_iota(jnp.int32, (8, 8), 0)
                == lax.broadcasted_iota(jnp.int32, (8, 8), 1))

    def by_head(row):
        return jnp.sum(jnp.where(diagonal, jnp.broadcast_to(row, (8, 8)), 0.0), axis=1, keepdims=True)

    cb0 = jnp.broadcast_to(by_head(cbias[0:1, :]), (8, 128))
    cb1 = jnp.broadcast_to(by_head(cbias[1:2, :]), (8, 128))
    row_chain = jnp.broadcast_to(chain[pl.ds(seq, 1), :], (8, 128))
    my_chain = jnp.broadcast_to(chain[pl.ds(lax.div(dap, 32), 1), :], (8, 128))
    lane = lax.broadcasted_iota(jnp.int32, (8, 128), 1) - lax.rem(dap, 32) * 4
    terms = []
    for j in range(4):
        own_chain = jnp.sum(jnp.where(lane == j, my_chain, 0).astype(F32), axis=1, keepdims=True)
        terms.append(jnp.where(row_chain.astype(F32) == own_chain, cb0, cb1))
    with jax.named_scope("waitpair"):
        l_pair.wait()
    xs[...] = layer_norm(pair[...].astype(F32))
    l_bproj.wait()
    w_top = bproj[...].astype(BF16).astype(F32)
    w_both = jnp.concatenate([w_top, bproj[...] - w_top], axis=0).astype(BF16)

    def across(v):
        return lax.dot_general(w_both, v, (((1,), (1,)), ((), ())), preferred_element_type=F32)

    parts = []
    for j in range(4):
        xj = xs[pl.ds(j, 128, stride=4), :]
        high = xj.astype(BF16)
        low = (xj - high.astype(F32)).astype(BF16)
        pj = across(high) + across(low)
        parts.append(pj[:8] + pj[8:] + terms[j])
    mine[...] = jnp.concatenate(parts, axis=0).astype(BF16)
    zbuf[g] = mine[...]
    l_hom.wait()
    l_mrow.wait()
    l_mcol.wait()
    qbd[...] = jnp.zeros_like(qbd)

    with jax.named_scope("barrier"):
        pl.semaphore_wait(barrier, 25)

    def z_copy(n):
        zz = lax.rem(lax.div(z, 4) + n[0], 2) * 4 + lax.rem(z + n[1], 4)
        device = {"dap_0": zz, "dap_1": lax.rem(y + n[2], 2)}
        return remote(mine, zbuf.at[g], z_s, z_r.at[lax.div(z, 4)], device)

    def hom_copy(p):
        to = lax.rem(seq + p, 4)
        return remote(homall.at[seq], homall.at[seq], hom_s, hom_r.at[seq], {"seq": to})

    def hom_recv(p):
        fr = lax.rem(seq + p, 4)
        return remote(homall.at[fr], homall.at[fr], hom_s, hom_r.at[fr], {"seq": fr})

    def mrow_copy(p):
        to = lax.rem(seq + p, 4)
        return remote(mrow.at[seq], mrow.at[seq], mrow_s, mrow_r, {"seq": to})

    def mz_copy(n):
        to, device = far(n)
        return remote(mzb.at[g], mzb.at[g], mz_s, mz_r, device)

    def mp_copy(n):
        to, device = near(n)
        return remote(mzb, mcol.at[q], mp_s, mp_r, device)

    def drain(ref, sem):
        pltpu.make_async_copy(ref, ref, sem).wait()

    for n in HALVES:
        z_copy(n).start()
    for p in (2, 1, 3):
        mrow_copy(p).start()
    for p in (2, 1, 3):
        hom_copy(p).start()
    for n in FAR:
        mz_copy(n).start()

    def transposed(v):
        return v.astype(BF16).T

    def spread_queries(qt):
        for h in range(HEADS):
            qbd[h * 32:(h + 1) * 32, h * 128:(h + 1) * 128] = qt[h * 32:(h + 1) * 32, :]

    ri = lax.broadcasted_iota(jnp.int32, (128, 128), 0)
    ci = lax.broadcasted_iota(jnp.int32, (128, 128), 1)
    source = ((ri >> 3) & 1) * 64 + ((ri >> 2) & 1) * 32 + (ri >> 4) * 4 + (ri & 3)
    order = (ci == source).astype(BF16)

    def ordered(v):
        return mm(order, v).astype(BF16)

    def place(ref, b, v):
        rows = pl.ds(pl.multiple_of(lax.rem(b, 2) * 16, 16), 16)
        ref[lax.div(b, 2), :, rows, :] = v.reshape(8, 16, v.shape[-1])

    def block_scores(b, s, values):
        seen = mm(order, jnp.broadcast_to(mrow[b].astype(F32), (128, 128)).T.astype(BF16)) > 0.0
        s = [jnp.where(seen, s[:, h * 128:(h + 1) * 128] * SCALE, -1e30) for h in range(HEADS)]
        place(scores, b, jnp.concatenate(s, axis=1))
        place(vrow, b, values)

    l_wh.wait()
    own = homall[seq].astype(F32)
    with jax.named_scope("ownqkv"):
        normed = layer_norm(own).astype(BF16)
        qg = mm(normed, wh[...])
        spread_queries(transposed(qg[:, :WIDE]))
        gt[...] = transposed(qg[:, 3 * WIDE:]).astype(F32)
        kv = mm(ordered(normed), wh[:, WIDE:3 * WIDE])
        block_scores(seq, mm(kv[:, :WIDE].astype(BF16), qbd[...]), kv[:, WIDE:])

    def neighbour_blocks():
        drain(mrow.at[pl.ds(0, 3)], mrow_r)
        blocks = [lax.rem(seq + p, 4) for p in (1, 3, 2)]
        for p in (1, 3, 2):
            with jax.named_scope(f"hom{p}"):
                hom_recv(p).wait_recv()
        with jax.named_scope("nb"):
            normed = [ordered(layer_norm(homall[b].astype(F32)).astype(BF16)) for b in blocks]
            kv = mm(jnp.concatenate(normed, axis=0), wh[:, WIDE:3 * WIDE])
            s = mm(kv[:, :WIDE].astype(BF16), qbd[...])
            for n, b in enumerate(blocks):
                block_scores(b, s[n * 128:(n + 1) * 128], kv[n * 128:(n + 1) * 128, WIDE:])
            vt[...] = vrow[...].reshape(512, WIDE).astype(BF16).T

    partner = {"dap_3": 1 - c}

    def wave_copy(e, n):
        xx, half = lax.rem(x + n[0], 4), (1 - c if n[0] == 0 else n[1])
        device = {"dap_2": xx, "dap_3": half}
        return remote(pack.at[e, half], biasall.at[half, e, q], wave_s.at[e], wave_r.at[e, q], device)

    first = lax.div(z, 4)
    second = 1 - first

    def wave_send(e, count):
        with jax.named_scope(f"zwait{count}"):
            drain(zbuf.at[pl.ds(0, count)], z_r.at[e])
        xs[:256, :] = zbuf[pl.ds(e * 8, 8)].reshape(256, 128).astype(F32)
        for h in range(HEADS):
            pack[e, h // 4, :, (h % 4) * 128:(h % 4 + 1) * 128] = xs[pl.ds(h, 32, stride=8), :].astype(BF16)
        biasall[c, e, q] = pack[e, c]
        for n in WAVE:
            wave_copy(e, n).start()

    def pass_on(e, block):
        remote(biasall.at[c, e, block], biasall.at[c, e, block], part_s.at[e], part_r.at[e], partner).start()

    def hand_over(e, n):
        pass_on(e, q)
        with jax.named_scope(f"wave{n}"):
            for m in reversed(NEAR):
                block = near(m)[0]
                drain(biasall.at[0, 0, 0], wave_r.at[e, block])
                pass_on(e, block)

    wave_send(first, 7)
    wave_send(second, 8)
    hand_over(first, 0)
    neighbour_blocks()

    def half_scores(e, half, h):
        lanes = pl.ds(pl.multiple_of((half * 4 + h) * 128, 128), 128)
        s = scores[e, :, :, lanes].reshape(256, 128)
        return s + biasall[half, e, :, :, h * 128:(h + 1) * 128].reshape(256, 128).astype(F32)

    def first_half(half):
        for h in range(4):
            s = half_scores(first, half, h)
            m = jnp.max(s, axis=0, keepdims=True)
            e = jnp.exp(s - m)
            scores[first, :, :, pl.ds(pl.multiple_of((half * 4 + h) * 128, 128), 128)] = e.reshape(8, 32, 128)
            top[half * 4 + h] = m
            total[half * 4 + h] = jnp.sum(e, axis=0, keepdims=True)

    def second_half(half):
        for h in range(4):
            head = half * 4 + h
            s = half_scores(second, half, h)
            m = jnp.maximum(top[head], jnp.max(s, axis=0, keepdims=True))
            e = jnp.exp(s - m)
            before = jnp.exp(top[head] - m)
            share = 1.0 / (total[head] * before + jnp.sum(e, axis=0, keepdims=True))
            old = scores[first, :, :, pl.ds(pl.multiple_of(head * 128, 128), 128)].reshape(256, 128)
            rows = pl.ds(pl.multiple_of(head * 32, 32), 32)
            ot[rows, :] = (
                mm(vt[rows, pl.ds(pl.multiple_of(first * 256, 256), 256)], (old * (before * share)).astype(BF16))
                + mm(vt[rows, pl.ds(pl.multiple_of(second * 256, 256), 256)], (e * share).astype(BF16)))

    with jax.named_scope("half1"):
        first_half(c)

    def partner_first_half():
        drain(biasall.at[1 - c, 0], part_r.at[first])
        first_half(1 - c)

    @pl.when(c == 0)
    def _():
        partner_first_half()

    hand_over(second, 1)

    @pl.when(c == 1)
    def _():
        partner_first_half()

    with jax.named_scope("rowattn"):
        second_half(c)
    with jax.named_scope("partner"):
        drain(biasall.at[1 - c, 0], part_r.at[second])
    with jax.named_scope("rowattn2"):
        second_half(1 - c)

    def softmax_out(s, vth):
        m = jnp.max(s, axis=0, keepdims=True)
        e = jnp.exp(s - m)
        w = (e * (1.0 / jnp.sum(e, axis=0, keepdims=True))).astype(BF16)
        return mm(vth, w)

    def pairs(v):
        fs[pl.ds(0, 128, stride=2), :] = v[:, :128]
        fs[pl.ds(1, 128, stride=2), :] = v[:, 128:]
        return fs[...].astype(BF16).reshape(128, 2, 128)

    def unpaired(v):
        fs[...] = v.reshape(256, 128).astype(F32)
        return jnp.concatenate([fs[pl.ds(0, 128, stride=2), :], fs[pl.ds(1, 128, stride=2), :]], axis=1)

    mine_row = q * 16 + g

    def exchange(copy):
        def rest(dz, dims):
            for dx, dy, dc in dims:
                to_g = lax.rem(z + dz, 8) * 2 + lax.rem(y + dy, 2)
                to_q = lax.rem(x + dx, 4) * 2 + lax.rem(c + dc, 2)
                copy(to_g, to_q, {
                    "dap_0": lax.rem(z + dz, 8), "dap_1": lax.rem(y + dy, 2),
                    "dap_2": lax.rem(x + dx, 4), "dap_3": lax.rem(c + dc, 2)}).start()

        @pl.loop(0, 7)
        def _(n):
            rest(4 + lax.div(n + 1, 2) * (1 - 2 * lax.rem(n, 2)), ALL)

        rest(0, ALL[:-1])

    def gated_project(w):
        g = (jax.nn.sigmoid(gt[...]) * ot[...]).astype(BF16)
        return mm(g.T, w)

    with jax.named_scope("rowproj"):
        l_rest[0].wait()
        one = homall[seq].astype(F32) + gated_project(ph[...])
        a1s[...] = pairs(one)
        a1[mine_row] = a1s[dap]

    def a1_copy(to_g, to_q, device):
        return remote(a1s.at[to_g * 8 + to_q], a1.at[mine_row], a1_s, a1_r, device)

    exchange(a1_copy)
    drain(mzb.at[pl.ds(0, 15)], mz_r)
    for n in NEAR:
        mp_copy(n).start()
    mcol[q] = mzb[...]
    for ld in l_rest[1:]:
        ld.wait()
    with jax.named_scope("keepc"):
        drain(mcol.at[pl.ds(0, 7)], mp_r)
        pick = (ri == dap).astype(BF16)
        keepc[...] = mm(mcol[...].reshape(128, 128).astype(F32).astype(BF16), pick)
    with jax.named_scope("waita1"):
        drain(a1.at[pl.ds(0, 127)], a1_r)

    with jax.named_scope("colattn"):
        col = unpaired(a1[...])
        qkvg = mm(layer_norm(col).astype(BF16), wc[...])
        spread_queries(transposed(qkvg[:, :WIDE]))
        gt[...] = transposed(qkvg[:, 3 * WIDE:]).astype(F32)
        cs = mm(qkvg[:, WIDE:2 * WIDE].astype(BF16), qbd[...]) * SCALE
        cvt = transposed(qkvg[:, 2 * WIDE:3 * WIDE])
        for h in range(HEADS):
            s = jnp.where(keepc[...] > 0.0, cs[:, h * 128:(h + 1) * 128], -1000000000.0)
            ot[h * 32:(h + 1) * 32, :] = softmax_out(s, cvt[h * 32:(h + 1) * 32, :])
    with jax.named_scope("transition"):
        two = col + gated_project(pv[...])
        inner = jnp.maximum(mm(layer_norm(two).astype(BF16), ex[...]), 0.0).astype(BF16)
        done = two + mm(inner, co[...])
        b1s[...] = pairs(done)
        b2[dap] = b1s[mine_row]

    def b2_copy(to_g, to_q, device):
        return remote(b1s.at[to_q * 16 + to_g], b2.at[dap], b2_s, b2_r, device)

    exchange(b2_copy)

    drain(zbuf.at[pl.ds(0, 15)], z_s)
    for e in range(2):
        drain(biasall.at[0, 0, pl.ds(0, 7)], wave_s.at[e])
    drain(mcol.at[pl.ds(0, 7)], mp_s)
    drain(a1.at[pl.ds(0, 127)], a1_s)
    drain(mzb.at[pl.ds(0, 15)], mz_s)
    drain(homall.at[pl.ds(0, 3)], hom_s)
    drain(mrow.at[pl.ds(0, 3)], mrow_s)
    for e in range(2):
        drain(biasall.at[0, 0], part_s.at[e])
    with jax.named_scope("waitb2"):
        drain(b2.at[pl.ds(0, 127)], b2_r)
    drain(b2.at[pl.ds(0, 127)], b2_s)
    out[...] = unpaired(b2[...]).astype(BF16)


def body(
    homolog_tensor, pair_features, entry_real_mask, chain_ids, horizontal_matrices,
    horizontal_projector, bias_proj, chain_bias, column_proj, vertical_projector,
    expansion_matrix, contraction_matrix,
):
    vmem = pl.BlockSpec(memory_space=pltpu.VMEM)
    hbm = pl.BlockSpec(memory_space=pl.ANY)
    dma = pltpu.SemaphoreType.DMA
    updated = pl.pallas_call(
        kernel,
        name="msa_block",
        out_shape=pltpu.VMEM((128, WIDE), BF16),
        in_specs=[hbm] * 12,
        out_specs=vmem,
        scratch_shapes=[
            pltpu.VMEM((512, 128), BF16),
            pltpu.VMEM((4, 128), jnp.int32),
            pltpu.VMEM((8, 128), F32),
            pltpu.VMEM((2, 8), F32),
            pltpu.VMEM((WIDE, 4 * WIDE), BF16),
            pltpu.VMEM((WIDE, WIDE), BF16),
            pltpu.VMEM((WIDE, 4 * WIDE), BF16),
            pltpu.VMEM((WIDE, WIDE), BF16),
            pltpu.VMEM((WIDE, 4 * WIDE), BF16),
            pltpu.VMEM((4 * WIDE, WIDE), BF16),
            pltpu.VMEM((512, 128), F32),
            pltpu.VMEM((32, 128), BF16),
            pltpu.VMEM((16, 32, 128), BF16),
            pltpu.VMEM((2, 2, 32, 512), BF16),
            pltpu.VMEM((2, 2, 8, 32, 512), BF16),
            pltpu.VMEM((4, 128, WIDE), BF16),
            pltpu.VMEM((4, 1, 128), jnp.int32),
            pltpu.VMEM((16, 1, 128), jnp.int32),
            pltpu.VMEM((8, 16, 1, 128), jnp.int32),
            pltpu.VMEM((128, 128), F32),
            pltpu.VMEM((WIDE, 1024), BF16),
            pltpu.VMEM((2, 8, 32, WIDE), F32),
            pltpu.VMEM((WIDE, 512), BF16),
            pltpu.VMEM((2, 8, 32, 1024), F32),
            pltpu.VMEM((8, 1, 128), F32),
            pltpu.VMEM((8, 1, 128), F32),
            pltpu.VMEM((WIDE, 128), F32),
            pltpu.VMEM((WIDE, 128), F32),
            pltpu.VMEM((128, 2, 128), BF16),
            pltpu.VMEM((128, 2, 128), BF16),
            pltpu.VMEM((128, 2, 128), BF16),
            pltpu.VMEM((128, 2, 128), BF16),
            pltpu.VMEM((256, 128), F32),
            dma((13,)), dma, dma((2,)), dma, dma((4,)), dma, dma, dma, dma, dma, dma,
            dma((2,)), dma((2, 8)), dma((2,)), dma((2,)), dma, dma, dma, dma,
        ],
        compiler_params=pltpu.CompilerParams(collective_id=0, has_side_effects=True),
    )(
        homolog_tensor.reshape(128, WIDE),
        pair_features.reshape(512, 128),
        entry_real_mask,
        chain_ids.reshape(4, 128),
        bias_proj.T,
        chain_bias,
        horizontal_matrices,
        horizontal_projector,
        column_proj,
        vertical_projector,
        expansion_matrix,
        contraction_matrix,
    )
    return updated.reshape(1, 128, WIDE)


def solution(mesh):
    torus = Mesh(
        mesh.devices.reshape(8, 2, 4, 2, mesh.shape["seq"]),
        ("dap_0", "dap_1", "dap_2", "dap_3", "seq"),
    )
    return jax.shard_map(
        body,
        mesh=torus,
        in_specs=(P(DAP, "seq", None), P("seq", DAP, None), P(DAP, "seq")) + (P(),) * 9,
        out_specs=P(DAP, "seq", None),
        check_vma=False,
    )
```

```python
import jax
import jax.numpy as jnp
from jax import lax
from jax.experimental import pallas as pl
from jax.experimental.pallas import tpu as pltpu
from jax.sharding import Mesh
from jax.sharding import PartitionSpec as P

HEADS = 8
DEPTH = 32
WIDE = 256
SCALE = DEPTH ** (-0.5)
EPS = 1e-05
DAP = ("dap_0", "dap_1", "dap_2", "dap_3")
MESH = pl.DeviceIdType.MESH
F32 = jnp.float32
BF16 = jnp.bfloat16


def layer_norm(x):
    center = x - jnp.mean(x, axis=-1, keepdims=True)
    spread = jnp.mean(center * center, axis=-1, keepdims=True)
    return center * lax.rsqrt(spread + EPS)


def mm(a, b):
    return jnp.dot(a, b, preferred_element_type=F32)


FAR = tuple((dz, dy) for dz in (4, 3, 5, 2, 6, 1, 7, 0) for dy in (1, 0) if dz or dy)
PAIRS = tuple((o, i, dy) for o in (0, 1, 3, 2) for i in (1, 0) for dy in range(2) if o or i or dy)
WAVE = tuple((dx, core) for core in range(2) for dx in (2, 1, 3)) + ((0, 0),)
ALL = tuple((dx, dy, dc) for dx in (2, 1, 3, 0) for dy in (1, 0) for dc in (1, 0))
NEAR = tuple((dx, dc) for dx in (2, 1, 3, 0) for dc in (1, 0) if dx or dc)


def kernel(
    hom_h, pair_h, mask_h, chain_h, bproj_h, cbias_h, wh_h, ph_h, wc_h, pv_h, ex_h, co_h,
    out,
    pair, chain, bproj, cbias, wh, ph, wc, pv, ex, co,
    xs, mine, zbuf, pack, biasall, homall, mrow, mzb, mcol, keepc,
    qbd, vrow, vt, scores, top, total, ot, gt,
    a1s, a1, b1s, b2, fs,
    lsem, z_s, z_r, hom_s, hom_r, mrow_s, mrow_r, mp_s, mp_r, mz_s, mz_r,
    wave_s, wave_r, last_r, part_s, part_r, a1_s, a1_r, b2_s, b2_r,
):
    z = lax.axis_index("dap_0")
    y = lax.axis_index("dap_1")
    x = lax.axis_index("dap_2")
    c = lax.axis_index("dap_3")
    seq = lax.axis_index("seq")
    g = z * 2 + y
    q = x * 2 + c
    dap = g * 8 + q

    def local(n, src, dst):
        return pltpu.make_async_copy(src, dst, lsem.at[n])

    l_pair = local(0, pair_h, pair)
    l_chain = local(1, chain_h, chain)
    l_bproj = local(2, bproj_h, bproj)
    l_cbias = local(3, cbias_h, cbias)
    l_hom = local(4, hom_h, homall.at[seq])
    l_mrow = local(5, mask_h, mrow.at[seq])
    l_mcol = local(6, mask_h, mzb.at[g])
    l_wh = local(7, wh_h, wh)
    l_rest = [local(8 + n, a, b) for n, (a, b) in enumerate(
        ((ph_h, ph), (wc_h, wc), (pv_h, pv), (ex_h, ex), (co_h, co)))]
    with jax.named_scope("start"):
        for ld in (l_pair, l_chain, l_cbias, l_bproj):
            ld.start()

    def remote(src, dst, ss, rs, device):
        return pltpu.make_async_remote_copy(
            src_ref=src, dst_ref=dst, send_sem=ss, recv_sem=rs, device_id=device,
            device_id_type=MESH)

    barrier = pltpu.get_barrier_semaphore()

    def far(n):
        zz, yy = lax.rem(z + n[0], 8), lax.rem(y + n[1], 2)
        return zz * 2 + yy, {"dap_0": zz, "dap_1": yy}

    def near(n):
        xx, cc = lax.rem(x + n[0], 4), lax.rem(c + n[1], 2)
        return xx * 2 + cc, {"dap_2": xx, "dap_3": cc}

    with jax.named_scope("signals"):
        for n in FAR:
            pl.semaphore_signal(barrier, inc=1, device_id=far(n)[1], device_id_type=MESH)
        for n in (2, 1, 3):
            pl.semaphore_signal(barrier, inc=1, device_id={"seq": lax.rem(seq + n, 4)}, device_id_type=MESH)
        for n in NEAR:
            pl.semaphore_signal(barrier, inc=1, device_id=near(n)[1], device_id_type=MESH)

    for ld in (l_hom, l_mrow, l_mcol):
        ld.start()
    l_wh.start()
    for ld in l_rest:
        ld.start()

    l_chain.wait()
    l_cbias.wait()
    diagonal = (lax.broadcasted_iota(jnp.int32, (8, 8), 0)
                == lax.broadcasted_iota(jnp.int32, (8, 8), 1))

    def by_head(row):
        return jnp.sum(jnp.where(diagonal, jnp.broadcast_to(row, (8, 8)), 0.0), axis=1, keepdims=True)

    cb0 = jnp.broadcast_to(by_head(cbias[0:1, :]), (8, 128))
    cb1 = jnp.broadcast_to(by_head(cbias[1:2, :]), (8, 128))
    row_chain = jnp.broadcast_to(chain[pl.ds(seq, 1), :], (8, 128))
    my_chain = jnp.broadcast_to(chain[pl.ds(lax.div(dap, 32), 1), :], (8, 128))
    lane = lax.broadcasted_iota(jnp.int32, (8, 128), 1) - lax.rem(dap, 32) * 4
    terms = []
    for j in range(4):
        own_chain = jnp.sum(jnp.where(lane == j, my_chain, 0).astype(F32), axis=1, keepdims=True)
        terms.append(jnp.where(row_chain.astype(F32) == own_chain, cb0, cb1))
    with jax.named_scope("waitpair"):
        l_pair.wait()
    xs[...] = layer_norm(pair[...].astype(F32))
    l_bproj.wait()
    w_top = bproj[...].astype(BF16).astype(F32)
    w_both = jnp.concatenate([w_top, bproj[...] - w_top], axis=0).astype(BF16)

    def across(v):
        return lax.dot_general(w_both, v, (((1,), (1,)), ((), ())), preferred_element_type=F32)

    parts = []
    for j in range(4):
        xj = xs[pl.ds(j, 128, stride=4), :]
        high = xj.astype(BF16)
        low = (xj - high.astype(F32)).astype(BF16)
        pj = across(high) + across(low)
        parts.append(pj[:8] + pj[8:] + terms[j])
    mine[...] = jnp.concatenate(parts, axis=0).astype(BF16)
    zbuf[g] = mine[...]
    l_hom.wait()
    l_mrow.wait()
    l_mcol.wait()
    qbd[...] = jnp.zeros_like(qbd)

    with jax.named_scope("barrier"):
        pl.semaphore_wait(barrier, 25)

    def z_copy(n):
        zz = lax.rem(lax.div(z, 2) + n[0], 4) * 2 + lax.rem(z + n[1], 2)
        device = {"dap_0": zz, "dap_1": lax.rem(y + n[2], 2)}
        return remote(mine, zbuf.at[g], z_s, z_r.at[lax.div(z, 2)], device)

    def hom_copy(p):
        to = lax.rem(seq + p, 4)
        return remote(homall.at[seq], homall.at[seq], hom_s, hom_r.at[seq], {"seq": to})

    def hom_recv(p):
        fr = lax.rem(seq + p, 4)
        return remote(homall.at[fr], homall.at[fr], hom_s, hom_r.at[fr], {"seq": fr})

    def mrow_copy(p):
        to = lax.rem(seq + p, 4)
        return remote(mrow.at[seq], mrow.at[seq], mrow_s, mrow_r, {"seq": to})

    def mz_copy(n):
        to, device = far(n)
        return remote(mzb.at[g], mzb.at[g], mz_s, mz_r, device)

    def mp_copy(n):
        to, device = near(n)
        return remote(mzb, mcol.at[q], mp_s, mp_r, device)

    def drain(ref, sem):
        pltpu.make_async_copy(ref, ref, sem).wait()

    for n in PAIRS:
        z_copy(n).start()
    for p in (2, 1, 3):
        mrow_copy(p).start()
    for p in (2, 1, 3):
        hom_copy(p).start()
    for n in FAR:
        mz_copy(n).start()

    def transposed(v):
        return v.astype(BF16).T

    def spread_queries(qt):
        for h in range(HEADS):
            qbd[h * 32:(h + 1) * 32, h * 128:(h + 1) * 128] = qt[h * 32:(h + 1) * 32, :]

    ri = lax.broadcasted_iota(jnp.int32, (128, 128), 0)
    ci = lax.broadcasted_iota(jnp.int32, (128, 128), 1)
    source = ((ri >> 3) & 1) * 64 + ((ri >> 2) & 1) * 32 + (ri >> 4) * 4 + (ri & 3)
    order = (ci == source).astype(BF16)

    def ordered(v):
        return mm(order, v).astype(BF16)

    def place(ref, b, v):
        ref[b] = v.reshape(8, 16, v.shape[-1])

    def block_scores(b, s, values):
        seen = mm(order, jnp.broadcast_to(mrow[b].astype(F32), (128, 128)).T.astype(BF16)) > 0.0
        s = [jnp.where(seen, s[:, h * 128:(h + 1) * 128] * SCALE, -1e30) for h in range(HEADS)]
        place(scores, b, jnp.concatenate(s, axis=1))
        place(vrow, b, values)

    l_wh.wait()
    own = homall[seq].astype(F32)
    with jax.named_scope("ownqkv"):
        normed = layer_norm(own).astype(BF16)
        qg = mm(normed, wh[...])
        spread_queries(transposed(qg[:, :WIDE]))
        gt[...] = transposed(qg[:, 3 * WIDE:]).astype(F32)
        kv = mm(ordered(normed), wh[:, WIDE:3 * WIDE])
        block_scores(seq, mm(kv[:, :WIDE].astype(BF16), qbd[...]), kv[:, WIDE:])

    def neighbour_blocks():
        drain(mrow.at[pl.ds(0, 3)], mrow_r)
        blocks = [lax.rem(seq + p, 4) for p in (1, 3, 2)]
        for p in (1, 3, 2):
            with jax.named_scope(f"hom{p}"):
                hom_recv(p).wait_recv()
        with jax.named_scope("nb"):
            normed = [ordered(layer_norm(homall[b].astype(F32)).astype(BF16)) for b in blocks]
            kv = mm(jnp.concatenate(normed, axis=0), wh[:, WIDE:3 * WIDE])
            s = mm(kv[:, :WIDE].astype(BF16), qbd[...])
            for n, b in enumerate(blocks):
                block_scores(b, s[n * 128:(n + 1) * 128], kv[n * 128:(n + 1) * 128, WIDE:])
            vt[...] = vrow[...].reshape(512, WIDE).astype(BF16).T

    partner = {"dap_3": 1 - c}

    def wave_copy(n, to):
        e = waves[n]
        xx, half = lax.rem(x + to[0], 4), (1 - c if to[0] == 0 else to[1])
        device = {"dap_2": xx, "dap_3": half}
        arrived = wave_r.at[n] if n < 3 else last_r.at[q]
        return remote(pack.at[e, half], biasall.at[half, e, q], wave_s, arrived, device)

    waves = [lax.rem(lax.div(z, 2) + o, 4) for o in (0, 1, 3, 2)]

    def wave_send(n, count):
        e = waves[n]
        with jax.named_scope(f"zwait{n}"):
            drain(zbuf.at[pl.ds(0, count)], z_r.at[e])
        xs[:128, :] = zbuf[pl.ds(e * 4, 4)].reshape(128, 128).astype(F32)
        for h in range(HEADS):
            pack[e, h // 4, :, (h % 4) * 128:(h % 4 + 1) * 128] = xs[pl.ds(h, 16, stride=8), :].astype(BF16)
        biasall[c, e, q] = pack[e, c]
        for to in WAVE:
            wave_copy(n, to).start()

    def pass_on(n, ref):
        remote(ref, ref, part_s, part_r.at[n], partner).start()

    def hand_over(n):
        e = waves[n]
        with jax.named_scope(f"wave{n}"):
            if n < 3:
                drain(biasall.at[0, 0, pl.ds(0, 7)], wave_r.at[n])
                pass_on(n, biasall.at[c, e])
            else:
                pass_on(n, biasall.at[c, e, q])
                for m in reversed(NEAR):
                    block = near(m)[0]
                    drain(biasall.at[0, 0, 0], last_r.at[block])
                    pass_on(n, biasall.at[c, e, block])

    wave_send(0, 3)
    for n in range(1, 4):
        wave_send(n, 4)
    hand_over(0)
    neighbour_blocks()
    hand_over(1)
    hand_over(2)

    def wave_scores(e, half, h):
        lanes = pl.ds(pl.multiple_of((half * 4 + h) * 128, 128), 128)
        s = scores[e, :, :, lanes].reshape(128, 128)
        return s + biasall[half, e, :, :, h * 128:(h + 1) * 128].reshape(128, 128).astype(F32)

    def first_part(half):
        for h in range(4):
            s = [wave_scores(e, half, h) for e in waves[:3]]
            m = jnp.max(jnp.maximum(jnp.maximum(s[0], s[1]), s[2]), axis=0, keepdims=True)
            p = [jnp.exp(v - m) for v in s]
            for e, v in zip(waves, p):
                scores[e, :, :, pl.ds(pl.multiple_of((half * 4 + h) * 128, 128), 128)] = v.reshape(8, 16, 128)
            top[half * 4 + h] = m
            total[half * 4 + h] = jnp.sum(p[0] + p[1] + p[2], axis=0, keepdims=True)

    def last_part(half):
        for h in range(4):
            head = half * 4 + h
            rows = pl.ds(pl.multiple_of(head * 32, 32), 32)
            s = wave_scores(waves[3], half, h)
            m = jnp.maximum(top[head], jnp.max(s, axis=0, keepdims=True))
            p = jnp.exp(s - m)
            before = jnp.exp(top[head] - m)
            share = 1.0 / (total[head] * before + jnp.sum(p, axis=0, keepdims=True))
            lanes = pl.ds(pl.multiple_of(head * 128, 128), 128)
            parts = [scores[e, :, :, lanes].reshape(128, 128) * (before * share) for e in waves[:3]] + [p * share]
            ot[rows, :] = sum(
                mm(vt[rows, pl.ds(pl.multiple_of(e * 128, 128), 128)], v.astype(BF16))
                for e, v in zip(waves, parts))

    with jax.named_scope("half1"):
        first_part(c)

    hand_over(3)
    with jax.named_scope("rowattn"):
        last_part(c)
    with jax.named_scope("partner0"):
        for n in range(3):
            drain(biasall.at[1 - c, 0], part_r.at[n])
    with jax.named_scope("half1b"):
        first_part(1 - c)
    with jax.named_scope("partner"):
        drain(biasall.at[1 - c, 0], part_r.at[3])
    with jax.named_scope("rowattn2"):
        last_part(1 - c)

    def softmax_out(s, vth):
        m = jnp.max(s, axis=0, keepdims=True)
        e = jnp.exp(s - m)
        w = (e * (1.0 / jnp.sum(e, axis=0, keepdims=True))).astype(BF16)
        return mm(vth, w)

    def pairs(v):
        fs[pl.ds(0, 128, stride=2), :] = v[:, :128]
        fs[pl.ds(1, 128, stride=2), :] = v[:, 128:]
        return fs[...].astype(BF16).reshape(128, 2, 128)

    def unpaired(v):
        fs[...] = v.reshape(256, 128).astype(F32)
        return jnp.concatenate([fs[pl.ds(0, 128, stride=2), :], fs[pl.ds(1, 128, stride=2), :]], axis=1)

    mine_row = q * 16 + g

    def exchange(copy):
        def rest(dz, dims):
            for dx, dy, dc in dims:
                to_g = lax.rem(z + dz, 8) * 2 + lax.rem(y + dy, 2)
                to_q = lax.rem(x + dx, 4) * 2 + lax.rem(c + dc, 2)
                copy(to_g, to_q, {
                    "dap_0": lax.rem(z + dz, 8), "dap_1": lax.rem(y + dy, 2),
                    "dap_2": lax.rem(x + dx, 4), "dap_3": lax.rem(c + dc, 2)}).start()

        @pl.loop(0, 7)
        def _(n):
            rest(4 + lax.div(n + 1, 2) * (1 - 2 * lax.rem(n, 2)), ALL)

        rest(0, ALL[:-1])

    def gated_project(w):
        g = (jax.nn.sigmoid(gt[...]) * ot[...]).astype(BF16)
        return mm(g.T, w)

    with jax.named_scope("rowproj"):
        l_rest[0].wait()
        one = homall[seq].astype(F32) + gated_project(ph[...])
        a1s[...] = pairs(one)
        a1[mine_row] = a1s[dap]

    def a1_copy(to_g, to_q, device):
        return remote(a1s.at[to_g * 8 + to_q], a1.at[mine_row], a1_s, a1_r, device)

    exchange(a1_copy)
    drain(mzb.at[pl.ds(0, 15)], mz_r)
    for n in NEAR:
        mp_copy(n).start()
    mcol[q] = mzb[...]
    for ld in l_rest[1:]:
        ld.wait()
    with jax.named_scope("keepc"):
        drain(mcol.at[pl.ds(0, 7)], mp_r)
        pick = (ri == dap).astype(BF16)
        keepc[...] = mm(mcol[...].reshape(128, 128).astype(F32).astype(BF16), pick)
    with jax.named_scope("waita1"):
        drain(a1.at[pl.ds(0, 127)], a1_r)

    with jax.named_scope("colattn"):
        col = unpaired(a1[...])
        qkvg = mm(layer_norm(col).astype(BF16), wc[...])
        spread_queries(transposed(qkvg[:, :WIDE]))
        gt[...] = transposed(qkvg[:, 3 * WIDE:]).astype(F32)
        cs = mm(qkvg[:, WIDE:2 * WIDE].astype(BF16), qbd[...]) * SCALE
        cvt = transposed(qkvg[:, 2 * WIDE:3 * WIDE])
        for h in range(HEADS):
            s = jnp.where(keepc[...] > 0.0, cs[:, h * 128:(h + 1) * 128], -1000000000.0)
            ot[h * 32:(h + 1) * 32, :] = softmax_out(s, cvt[h * 32:(h + 1) * 32, :])
    with jax.named_scope("transition"):
        two = col + gated_project(pv[...])
        inner = jnp.maximum(mm(layer_norm(two).astype(BF16), ex[...]), 0.0).astype(BF16)
        done = two + mm(inner, co[...])
        b1s[...] = pairs(done)
        b2[dap] = b1s[mine_row]

    def b2_copy(to_g, to_q, device):
        return remote(b1s.at[to_q * 16 + to_g], b2.at[dap], b2_s, b2_r, device)

    exchange(b2_copy)

    drain(zbuf.at[pl.ds(0, 15)], z_s)
    drain(wh.at[pl.ds(0, 224)], wave_s)
    drain(mcol.at[pl.ds(0, 7)], mp_s)
    drain(a1.at[pl.ds(0, 127)], a1_s)
    drain(mzb.at[pl.ds(0, 15)], mz_s)
    drain(homall.at[pl.ds(0, 3)], hom_s)
    drain(mrow.at[pl.ds(0, 3)], mrow_s)
    drain(biasall.at[0], part_s)
    with jax.named_scope("waitb2"):
        drain(b2.at[pl.ds(0, 127)], b2_r)
    drain(b2.at[pl.ds(0, 127)], b2_s)
    out[...] = unpaired(b2[...]).astype(BF16)


def body(
    homolog_tensor, pair_features, entry_real_mask, chain_ids, horizontal_matrices,
    horizontal_projector, bias_proj, chain_bias, column_proj, vertical_projector,
    expansion_matrix, contraction_matrix,
):
    vmem = pl.BlockSpec(memory_space=pltpu.VMEM)
    hbm = pl.BlockSpec(memory_space=pl.ANY)
    dma = pltpu.SemaphoreType.DMA
    updated = pl.pallas_call(
        kernel,
        name="msa_block",
        out_shape=pltpu.VMEM((128, WIDE), BF16),
        in_specs=[hbm] * 12,
        out_specs=vmem,
        scratch_shapes=[
            pltpu.VMEM((512, 128), BF16),
            pltpu.VMEM((4, 128), jnp.int32),
            pltpu.VMEM((8, 128), F32),
            pltpu.VMEM((2, 8), F32),
            pltpu.VMEM((WIDE, 4 * WIDE), BF16),
            pltpu.VMEM((WIDE, WIDE), BF16),
            pltpu.VMEM((WIDE, 4 * WIDE), BF16),
            pltpu.VMEM((WIDE, WIDE), BF16),
            pltpu.VMEM((WIDE, 4 * WIDE), BF16),
            pltpu.VMEM((4 * WIDE, WIDE), BF16),
            pltpu.VMEM((512, 128), F32),
            pltpu.VMEM((32, 128), BF16),
            pltpu.VMEM((16, 32, 128), BF16),
            pltpu.VMEM((4, 2, 16, 512), BF16),
            pltpu.VMEM((2, 4, 8, 16, 512), BF16),
            pltpu.VMEM((4, 128, WIDE), BF16),
            pltpu.VMEM((4, 1, 128), jnp.int32),
            pltpu.VMEM((16, 1, 128), jnp.int32),
            pltpu.VMEM((8, 16, 1, 128), jnp.int32),
            pltpu.VMEM((128, 128), F32),
            pltpu.VMEM((WIDE, 1024), BF16),
            pltpu.VMEM((4, 8, 16, WIDE), F32),
            pltpu.VMEM((WIDE, 512), BF16),
            pltpu.VMEM((4, 8, 16, 1024), F32),
            pltpu.VMEM((8, 1, 128), F32),
            pltpu.VMEM((8, 1, 128), F32),
            pltpu.VMEM((WIDE, 128), F32),
            pltpu.VMEM((WIDE, 128), F32),
            pltpu.VMEM((128, 2, 128), BF16),
            pltpu.VMEM((128, 2, 128), BF16),
            pltpu.VMEM((128, 2, 128), BF16),
            pltpu.VMEM((128, 2, 128), BF16),
            pltpu.VMEM((256, 128), F32),
            dma((13,)), dma, dma((4,)), dma, dma((4,)), dma, dma, dma, dma, dma, dma,
            dma, dma((3,)), dma((8,)), dma, dma((4,)), dma, dma, dma, dma,
        ],
        compiler_params=pltpu.CompilerParams(collective_id=0, has_side_effects=True),
    )(
        homolog_tensor.reshape(128, WIDE),
        pair_features.reshape(512, 128),
        entry_real_mask,
        chain_ids.reshape(4, 128),
        bias_proj.T,
        chain_bias,
        horizontal_matrices,
        horizontal_projector,
        column_proj,
        vertical_projector,
        expansion_matrix,
        contraction_matrix,
    )
    return updated.reshape(1, 128, WIDE)


def solution(mesh):
    torus = Mesh(
        mesh.devices.reshape(8, 2, 4, 2, mesh.shape["seq"]),
        ("dap_0", "dap_1", "dap_2", "dap_3", "seq"),
    )
    return jax.shard_map(
        body,
        mesh=torus,
        in_specs=(P(DAP, "seq", None), P("seq", DAP, None), P(DAP, "seq")) + (P(),) * 9,
        out_specs=P(DAP, "seq", None),
        check_vma=False,
    )
```

```python
import jax
import jax.numpy as jnp
from jax import lax
from jax.experimental import pallas as pl
from jax.experimental.pallas import tpu as pltpu
from jax.sharding import Mesh
from jax.sharding import PartitionSpec as P

HEADS = 8
DEPTH = 32
WIDE = 256
SCALE = DEPTH ** (-0.5)
EPS = 1e-05
DAP = ("dap_0", "dap_1", "dap_2", "dap_3")
MESH = pl.DeviceIdType.MESH
F32 = jnp.float32
BF16 = jnp.bfloat16


def layer_norm(x):
    center = x - jnp.mean(x, axis=-1, keepdims=True)
    spread = jnp.mean(center * center, axis=-1, keepdims=True)
    return center * lax.rsqrt(spread + EPS)


def mm(a, b):
    return jnp.dot(a, b, preferred_element_type=F32)


FAR = tuple((dz, dy) for dz in (4, 3, 5, 2, 6, 1, 7, 0) for dy in (1, 0) if dz or dy)
PAIRS = tuple((o, i, dy) for o in range(4) for i in (1, 0) for dy in range(2) if o or i or dy)
WAVE = tuple((dx, core) for core in range(2) for dx in (2, 1, 3)) + ((0, 0),)
ALL = tuple((dx, dy, dc) for dx in (2, 1, 3, 0) for dy in (1, 0) for dc in (1, 0))
NEAR = tuple((dx, dc) for dx in (2, 1, 3, 0) for dc in (1, 0) if dx or dc)


def kernel(
    hom_h, pair_h, mask_h, chain_h, bproj_h, cbias_h, wh_h, ph_h, wc_h, pv_h, ex_h, co_h,
    out,
    pair, chain, bproj, cbias, wh, ph, wc, pv, ex, co,
    xs, mine, zbuf, pack, biasall, homall, mrow, mzb, mcol, keepc,
    qbd, vrow, vt, scores, top, total, ot, gt,
    a1s, a1, b1s, b2, fs,
    lsem, z_s, z_r, hom_s, hom_r, mrow_s, mrow_r, mp_s, mp_r, mz_s, mz_r,
    wave_s, wave_r, last_r, part_s, part_r, a1_s, a1_r, b2_s, b2_r,
):
    z = lax.axis_index("dap_0")
    y = lax.axis_index("dap_1")
    x = lax.axis_index("dap_2")
    c = lax.axis_index("dap_3")
    seq = lax.axis_index("seq")
    g = z * 2 + y
    q = x * 2 + c
    dap = g * 8 + q

    def local(n, src, dst):
        return pltpu.make_async_copy(src, dst, lsem.at[n])

    l_pair = local(0, pair_h, pair)
    l_chain = local(1, chain_h, chain)
    l_bproj = local(2, bproj_h, bproj)
    l_cbias = local(3, cbias_h, cbias)
    l_hom = local(4, hom_h, homall.at[seq])
    l_mrow = local(5, mask_h, mrow.at[seq])
    l_mcol = local(6, mask_h, mzb.at[g])
    l_wh = local(7, wh_h, wh)
    l_rest = [local(8 + n, a, b) for n, (a, b) in enumerate(
        ((ph_h, ph), (wc_h, wc), (pv_h, pv), (ex_h, ex), (co_h, co)))]
    with jax.named_scope("start"):
        for ld in (l_pair, l_chain, l_cbias, l_bproj):
            ld.start()

    def remote(src, dst, ss, rs, device):
        return pltpu.make_async_remote_copy(
            src_ref=src, dst_ref=dst, send_sem=ss, recv_sem=rs, device_id=device,
            device_id_type=MESH)

    barrier = pltpu.get_barrier_semaphore()

    def far(n):
        zz, yy = lax.rem(z + n[0], 8), lax.rem(y + n[1], 2)
        return zz * 2 + yy, {"dap_0": zz, "dap_1": yy}

    def near(n):
        xx, cc = lax.rem(x + n[0], 4), lax.rem(c + n[1], 2)
        return xx * 2 + cc, {"dap_2": xx, "dap_3": cc}

    with jax.named_scope("signals"):
        for n in FAR:
            pl.semaphore_signal(barrier, inc=1, device_id=far(n)[1], device_id_type=MESH)
        for n in (2, 1, 3):
            pl.semaphore_signal(barrier, inc=1, device_id={"seq": lax.rem(seq + n, 4)}, device_id_type=MESH)
        for n in NEAR:
            pl.semaphore_signal(barrier, inc=1, device_id=near(n)[1], device_id_type=MESH)

    for ld in (l_hom, l_mrow, l_mcol):
        ld.start()
    l_wh.start()
    for ld in l_rest:
        ld.start()

    l_chain.wait()
    l_cbias.wait()
    diagonal = (lax.broadcasted_iota(jnp.int32, (8, 8), 0)
                == lax.broadcasted_iota(jnp.int32, (8, 8), 1))

    def by_head(row):
        return jnp.sum(jnp.where(diagonal, jnp.broadcast_to(row, (8, 8)), 0.0), axis=1, keepdims=True)

    cb0 = jnp.broadcast_to(by_head(cbias[0:1, :]), (8, 128))
    cb1 = jnp.broadcast_to(by_head(cbias[1:2, :]), (8, 128))
    row_chain = jnp.broadcast_to(chain[pl.ds(seq, 1), :], (8, 128))
    my_chain = jnp.broadcast_to(chain[pl.ds(lax.div(dap, 32), 1), :], (8, 128))
    lane = lax.broadcasted_iota(jnp.int32, (8, 128), 1) - lax.rem(dap, 32) * 4
    terms = []
    for j in range(4):
        own_chain = jnp.sum(jnp.where(lane == j, my_chain, 0).astype(F32), axis=1, keepdims=True)
        terms.append(jnp.where(row_chain.astype(F32) == own_chain, cb0, cb1))
    with jax.named_scope("waitpair"):
        l_pair.wait()
    xs[...] = layer_norm(pair[...].astype(F32))
    l_bproj.wait()
    w_top = bproj[...].astype(BF16).astype(F32)
    w_both = jnp.concatenate([w_top, bproj[...] - w_top], axis=0).astype(BF16)

    def across(v):
        return lax.dot_general(w_both, v, (((1,), (1,)), ((), ())), preferred_element_type=F32)

    parts = []
    for j in range(4):
        xj = xs[pl.ds(j, 128, stride=4), :]
        high = xj.astype(BF16)
        low = (xj - high.astype(F32)).astype(BF16)
        pj = across(high) + across(low)
        parts.append(pj[:8] + pj[8:] + terms[j])
    mine[...] = jnp.concatenate(parts, axis=0).astype(BF16)
    zbuf[g] = mine[...]
    l_hom.wait()
    l_mrow.wait()
    l_mcol.wait()
    qbd[...] = jnp.zeros_like(qbd)

    with jax.named_scope("barrier"):
        pl.semaphore_wait(barrier, 25)

    pair_z = lax.div(z, 2)
    other_z = pair_z + 1 - 2 * lax.rem(pair_z, 2)
    waves = [pair_z, other_z, lax.rem(pair_z + 2, 4), lax.rem(other_z + 2, 4)]

    def z_copy(n):
        zz = waves[n[0]] * 2 + lax.rem(z + n[1], 2)
        device = {"dap_0": zz, "dap_1": lax.rem(y + n[2], 2)}
        return remote(mine, zbuf.at[g], z_s, z_r.at[lax.div(z, 2)], device)

    def hom_copy(p):
        to = lax.rem(seq + p, 4)
        return remote(homall.at[seq], homall.at[seq], hom_s, hom_r.at[seq], {"seq": to})

    def hom_recv(p):
        fr = lax.rem(seq + p, 4)
        return remote(homall.at[fr], homall.at[fr], hom_s, hom_r.at[fr], {"seq": fr})

    def mrow_copy(p):
        to = lax.rem(seq + p, 4)
        return remote(mrow.at[seq], mrow.at[seq], mrow_s, mrow_r, {"seq": to})

    def mz_copy(n):
        to, device = far(n)
        return remote(mzb.at[g], mzb.at[g], mz_s, mz_r, device)

    def mp_copy(n):
        to, device = near(n)
        return remote(mzb, mcol.at[q], mp_s, mp_r, device)

    def drain(ref, sem):
        pltpu.make_async_copy(ref, ref, sem).wait()

    for n in PAIRS:
        z_copy(n).start()
    for p in (2, 1, 3):
        mrow_copy(p).start()
    for p in (2, 1, 3):
        hom_copy(p).start()
    for n in FAR:
        mz_copy(n).start()

    def transposed(v):
        return v.astype(BF16).T

    def spread_queries(qt):
        for h in range(HEADS):
            qbd[h * 32:(h + 1) * 32, h * 128:(h + 1) * 128] = qt[h * 32:(h + 1) * 32, :]

    ri = lax.broadcasted_iota(jnp.int32, (128, 128), 0)
    ci = lax.broadcasted_iota(jnp.int32, (128, 128), 1)
    source = ((ri >> 3) & 1) * 64 + ((ri >> 2) & 1) * 32 + (ri >> 4) * 4 + (ri & 3)
    order = (ci == source).astype(BF16)

    def ordered(v):
        return mm(order, v).astype(BF16)

    def place(ref, b, v):
        ref[b] = v.reshape(8, 16, v.shape[-1])

    def block_scores(b, s, values):
        seen = mm(order, jnp.broadcast_to(mrow[b].astype(F32), (128, 128)).T.astype(BF16)) > 0.0
        s = [jnp.where(seen, s[:, h * 128:(h + 1) * 128] * SCALE, -1e30) for h in range(HEADS)]
        place(scores, b, jnp.concatenate(s, axis=1))
        place(vrow, b, values)

    l_wh.wait()
    own = homall[seq].astype(F32)
    with jax.named_scope("ownqkv"):
        normed = layer_norm(own).astype(BF16)
        qg = mm(normed, wh[...])
        spread_queries(transposed(qg[:, :WIDE]))
        gt[...] = transposed(qg[:, 3 * WIDE:]).astype(F32)
        kv = mm(ordered(normed), wh[:, WIDE:3 * WIDE])
        block_scores(seq, mm(kv[:, :WIDE].astype(BF16), qbd[...]), kv[:, WIDE:])

    def neighbour_blocks():
        drain(mrow.at[pl.ds(0, 3)], mrow_r)
        blocks = [lax.rem(seq + p, 4) for p in (1, 3, 2)]
        for p in (1, 3, 2):
            with jax.named_scope(f"hom{p}"):
                hom_recv(p).wait_recv()
        with jax.named_scope("nb"):
            normed = [ordered(layer_norm(homall[b].astype(F32)).astype(BF16)) for b in blocks]
            kv = mm(jnp.concatenate(normed, axis=0), wh[:, WIDE:3 * WIDE])
            s = mm(kv[:, :WIDE].astype(BF16), qbd[...])
            for n, b in enumerate(blocks):
                block_scores(b, s[n * 128:(n + 1) * 128], kv[n * 128:(n + 1) * 128, WIDE:])
            vt[...] = vrow[...].reshape(512, WIDE).astype(BF16).T

    partner = {"dap_3": 1 - c}

    def wave_copy(n, to):
        e = waves[n]
        xx, half = lax.rem(x + to[0], 4), (1 - c if to[0] == 0 else to[1])
        device = {"dap_2": xx, "dap_3": half}
        arrived = wave_r.at[n] if n < 3 else last_r.at[q]
        return remote(pack.at[e, half], biasall.at[half, e, q], wave_s, arrived, device)

    def wave_send(n, count):
        e = waves[n]
        with jax.named_scope(f"zwait{n}"):
            drain(zbuf.at[pl.ds(0, count)], z_r.at[e])
        xs[:128, :] = zbuf[pl.ds(e * 4, 4)].reshape(128, 128).astype(F32)
        for h in range(HEADS):
            pack[e, h // 4, :, (h % 4) * 128:(h % 4 + 1) * 128] = xs[pl.ds(h, 16, stride=8), :].astype(BF16)
        biasall[c, e, q] = pack[e, c]
        for to in WAVE:
            wave_copy(n, to).start()

    def pass_on(n, ref):
        remote(ref, ref, part_s, part_r.at[n], partner).start()

    def hand_over(n):
        e = waves[n]
        with jax.named_scope(f"wave{n}"):
            if n < 3:
                drain(biasall.at[0, 0, pl.ds(0, 7)], wave_r.at[n])
                pass_on(n, biasall.at[c, e])
            else:
                pass_on(n, biasall.at[c, e, q])
                for m in reversed(NEAR):
                    block = near(m)[0]
                    drain(biasall.at[0, 0, 0], last_r.at[block])
                    pass_on(n, biasall.at[c, e, block])

    wave_send(0, 3)
    for n in range(1, 4):
        wave_send(n, 4)
    hand_over(0)
    neighbour_blocks()
    hand_over(1)
    hand_over(2)

    def wave_scores(e, half, h):
        lanes = pl.ds(pl.multiple_of((half * 4 + h) * 128, 128), 128)
        s = scores[e, :, :, lanes].reshape(128, 128)
        return s + biasall[half, e, :, :, h * 128:(h + 1) * 128].reshape(128, 128).astype(F32)

    def first_part(half):
        for h in range(4):
            s = [wave_scores(e, half, h) for e in waves[:3]]
            m = jnp.max(jnp.maximum(jnp.maximum(s[0], s[1]), s[2]), axis=0, keepdims=True)
            p = [jnp.exp(v - m) for v in s]
            for e, v in zip(waves, p):
                scores[e, :, :, pl.ds(pl.multiple_of((half * 4 + h) * 128, 128), 128)] = v.reshape(8, 16, 128)
            top[half * 4 + h] = m
            total[half * 4 + h] = jnp.sum(p[0] + p[1] + p[2], axis=0, keepdims=True)

    def last_part(half):
        for h in range(4):
            head = half * 4 + h
            rows = pl.ds(pl.multiple_of(head * 32, 32), 32)
            s = wave_scores(waves[3], half, h)
            m = jnp.maximum(top[head], jnp.max(s, axis=0, keepdims=True))
            p = jnp.exp(s - m)
            before = jnp.exp(top[head] - m)
            share = 1.0 / (total[head] * before + jnp.sum(p, axis=0, keepdims=True))
            lanes = pl.ds(pl.multiple_of(head * 128, 128), 128)
            parts = [scores[e, :, :, lanes].reshape(128, 128) * (before * share) for e in waves[:3]] + [p * share]
            ot[rows, :] = sum(
                mm(vt[rows, pl.ds(pl.multiple_of(e * 128, 128), 128)], v.astype(BF16))
                for e, v in zip(waves, parts))

    with jax.named_scope("half1"):
        first_part(c)

    hand_over(3)
    with jax.named_scope("rowattn"):
        last_part(c)
    with jax.named_scope("partner0"):
        for n in range(3):
            drain(biasall.at[1 - c, 0], part_r.at[n])
    with jax.named_scope("half1b"):
        first_part(1 - c)
    with jax.named_scope("partner"):
        drain(biasall.at[1 - c, 0], part_r.at[3])
    with jax.named_scope("rowattn2"):
        last_part(1 - c)

    def softmax_out(s, vth):
        m = jnp.max(s, axis=0, keepdims=True)
        e = jnp.exp(s - m)
        w = (e * (1.0 / jnp.sum(e, axis=0, keepdims=True))).astype(BF16)
        return mm(vth, w)

    def pairs(v):
        fs[pl.ds(0, 128, stride=2), :] = v[:, :128]
        fs[pl.ds(1, 128, stride=2), :] = v[:, 128:]
        return fs[...].astype(BF16).reshape(128, 2, 128)

    def unpaired(v):
        fs[...] = v.reshape(256, 128).astype(F32)
        return jnp.concatenate([fs[pl.ds(0, 128, stride=2), :], fs[pl.ds(1, 128, stride=2), :]], axis=1)

    mine_row = q * 16 + g

    def exchange(copy):
        def rest(dz, dims):
            for dx, dy, dc in dims:
                to_g = lax.rem(z + dz, 8) * 2 + lax.rem(y + dy, 2)
                to_q = lax.rem(x + dx, 4) * 2 + lax.rem(c + dc, 2)
                copy(to_g, to_q, {
                    "dap_0": lax.rem(z + dz, 8), "dap_1": lax.rem(y + dy, 2),
                    "dap_2": lax.rem(x + dx, 4), "dap_3": lax.rem(c + dc, 2)}).start()

        @pl.loop(0, 7)
        def _(n):
            rest(4 + lax.div(n + 1, 2) * (1 - 2 * lax.rem(n, 2)), ALL)

        rest(0, ALL[:-1])

    def gated_project(w):
        g = (jax.nn.sigmoid(gt[...]) * ot[...]).astype(BF16)
        return mm(g.T, w)

    with jax.named_scope("rowproj"):
        l_rest[0].wait()
        one = homall[seq].astype(F32) + gated_project(ph[...])
        a1s[...] = pairs(one)
        a1[mine_row] = a1s[dap]

    def a1_copy(to_g, to_q, device):
        return remote(a1s.at[to_g * 8 + to_q], a1.at[mine_row], a1_s, a1_r, device)

    exchange(a1_copy)
    drain(mzb.at[pl.ds(0, 15)], mz_r)
    for n in NEAR:
        mp_copy(n).start()
    mcol[q] = mzb[...]
    for ld in l_rest[1:]:
        ld.wait()
    with jax.named_scope("keepc"):
        drain(mcol.at[pl.ds(0, 7)], mp_r)
        pick = (ri == dap).astype(BF16)
        keepc[...] = mm(mcol[...].reshape(128, 128).astype(F32).astype(BF16), pick)
    with jax.named_scope("waita1"):
        drain(a1.at[pl.ds(0, 127)], a1_r)

    with jax.named_scope("colattn"):
        col = unpaired(a1[...])
        qkvg = mm(layer_norm(col).astype(BF16), wc[...])
        spread_queries(transposed(qkvg[:, :WIDE]))
        gt[...] = transposed(qkvg[:, 3 * WIDE:]).astype(F32)
        cs = mm(qkvg[:, WIDE:2 * WIDE].astype(BF16), qbd[...]) * SCALE
        cvt = transposed(qkvg[:, 2 * WIDE:3 * WIDE])
        for h in range(HEADS):
            s = jnp.where(keepc[...] > 0.0, cs[:, h * 128:(h + 1) * 128], -1000000000.0)
            ot[h * 32:(h + 1) * 32, :] = softmax_out(s, cvt[h * 32:(h + 1) * 32, :])
    with jax.named_scope("transition"):
        two = col + gated_project(pv[...])
        inner = jnp.maximum(mm(layer_norm(two).astype(BF16), ex[...]), 0.0).astype(BF16)
        done = two + mm(inner, co[...])
        b1s[...] = pairs(done)
        b2[dap] = b1s[mine_row]

    def b2_copy(to_g, to_q, device):
        return remote(b1s.at[to_q * 16 + to_g], b2.at[dap], b2_s, b2_r, device)

    exchange(b2_copy)

    drain(zbuf.at[pl.ds(0, 15)], z_s)
    drain(wh.at[pl.ds(0, 224)], wave_s)
    drain(mcol.at[pl.ds(0, 7)], mp_s)
    drain(a1.at[pl.ds(0, 127)], a1_s)
    drain(mzb.at[pl.ds(0, 15)], mz_s)
    drain(homall.at[pl.ds(0, 3)], hom_s)
    drain(mrow.at[pl.ds(0, 3)], mrow_s)
    drain(biasall.at[0], part_s)
    with jax.named_scope("waitb2"):
        drain(b2.at[pl.ds(0, 127)], b2_r)
    drain(b2.at[pl.ds(0, 127)], b2_s)
    out[...] = unpaired(b2[...]).astype(BF16)


def body(
    homolog_tensor, pair_features, entry_real_mask, chain_ids, horizontal_matrices,
    horizontal_projector, bias_proj, chain_bias, column_proj, vertical_projector,
    expansion_matrix, contraction_matrix,
):
    vmem = pl.BlockSpec(memory_space=pltpu.VMEM)
    hbm = pl.BlockSpec(memory_space=pl.ANY)
    dma = pltpu.SemaphoreType.DMA
    updated = pl.pallas_call(
        kernel,
        name="msa_block",
        out_shape=pltpu.VMEM((128, WIDE), BF16),
        in_specs=[hbm] * 12,
        out_specs=vmem,
        scratch_shapes=[
            pltpu.VMEM((512, 128), BF16),
            pltpu.VMEM((4, 128), jnp.int32),
            pltpu.VMEM((8, 128), F32),
            pltpu.VMEM((2, 8), F32),
            pltpu.VMEM((WIDE, 4 * WIDE), BF16),
            pltpu.VMEM((WIDE, WIDE), BF16),
            pltpu.VMEM((WIDE, 4 * WIDE), BF16),
            pltpu.VMEM((WIDE, WIDE), BF16),
            pltpu.VMEM((WIDE, 4 * WIDE), BF16),
            pltpu.VMEM((4 * WIDE, WIDE), BF16),
            pltpu.VMEM((512, 128), F32),
            pltpu.VMEM((32, 128), BF16),
            pltpu.VMEM((16, 32, 128), BF16),
            pltpu.VMEM((4, 2, 16, 512), BF16),
            pltpu.VMEM((2, 4, 8, 16, 512), BF16),
            pltpu.VMEM((4, 128, WIDE), BF16),
            pltpu.VMEM((4, 1, 128), jnp.int32),
            pltpu.VMEM((16, 1, 128), jnp.int32),
            pltpu.VMEM((8, 16, 1, 128), jnp.int32),
            pltpu.VMEM((128, 128), F32),
            pltpu.VMEM((WIDE, 1024), BF16),
            pltpu.VMEM((4, 8, 16, WIDE), F32),
            pltpu.VMEM((WIDE, 512), BF16),
            pltpu.VMEM((4, 8, 16, 1024), F32),
            pltpu.VMEM((8, 1, 128), F32),
            pltpu.VMEM((8, 1, 128), F32),
            pltpu.VMEM((WIDE, 128), F32),
            pltpu.VMEM((WIDE, 128), F32),
            pltpu.VMEM((128, 2, 128), BF16),
            pltpu.VMEM((128, 2, 128), BF16),
            pltpu.VMEM((128, 2, 128), BF16),
            pltpu.VMEM((128, 2, 128), BF16),
            pltpu.VMEM((256, 128), F32),
            dma((13,)), dma, dma((4,)), dma, dma((4,)), dma, dma, dma, dma, dma, dma,
            dma, dma((3,)), dma((8,)), dma, dma((4,)), dma, dma, dma, dma,
        ],
        compiler_params=pltpu.CompilerParams(collective_id=0, has_side_effects=True),
    )(
        homolog_tensor.reshape(128, WIDE),
        pair_features.reshape(512, 128),
        entry_real_mask,
        chain_ids.reshape(4, 128),
        bias_proj.T,
        chain_bias,
        horizontal_matrices,
        horizontal_projector,
        column_proj,
        vertical_projector,
        expansion_matrix,
        contraction_matrix,
    )
    return updated.reshape(1, 128, WIDE)


def solution(mesh):
    torus = Mesh(
        mesh.devices.reshape(8, 2, 4, 2, mesh.shape["seq"]),
        ("dap_0", "dap_1", "dap_2", "dap_3", "seq"),
    )
    return jax.shard_map(
        body,
        mesh=torus,
        in_specs=(P(DAP, "seq", None), P("seq", DAP, None), P(DAP, "seq")) + (P(),) * 9,
        out_specs=P(DAP, "seq", None),
        check_vma=False,
    )
```
